256 devices in a mesh: cols: 32 (over x, z_hi, y), params: 8 (over z_lo, core).
Axes of the slice: x: 4, y: 4, z: 8 (z_hi: 2, z_lo: 4; z = z_hi * 4 + z_lo), core: 2. Of those that a mesh axis runs over, the one named last changes fastest.
Arguments:
- concentration: float32 [128, 32768], P(None, ('cols', 'params')), may hold values from 0.2 to 5
- emissions: float32 [128, 32768], P(None, ('cols', 'params')), may hold values from 0 to 1
- rate_table: float32 [8, 16, 16], replicated, may hold values from 0.01 to 0.3
- species_order: int32 [128], replicated, may hold values from 0 to 127, each once
- sensitivity: float32 [16, 128, 64, 4, 128], P('params', None, 'cols'), may hold values from -6 to 6
- source_terms: bfloat16 [16, 128, 64, 4, 128], P('params', None, 'cols'), may hold values from 0 to 2
- courant_x: float32 [64, 4, 128], P('cols'), may hold values from 0.05 to 0.24
- upwind_x: int32 [64, 4, 128], P('cols'), may hold values from 0 to 1
- courant_y: float32 [64, 4, 128], P('cols'), may hold values from 0.05 to 0.24
- upwind_y: int32 [64, 4, 128], P('cols'), may hold values from 0 to 1
Outputs:
- new_concentration: float32 [128, 32768], P(None, ('cols', 'params'))
- new_sensitivity: float32 [16, 128, 64, 4, 128], P('params', None, 'cols')
- sensitivity_burden: float32 [16, 128], P('params')
- species_burden: float32 [128], replicated
The draws below stay inside these ranges and needn't reach their ends.
Inputs may be any that keep to these rules, and one draw needn't show every extreme that they name: `species_order`: each species appears exactly once. `upwind_x`: 1 means the wind blows toward higher indices through the face. `upwind_y`: 1 means the wind blows toward higher indices through the face.
All inputs are finite; a program needn't handle non-finite values.
Results may differ from the reference program's by a relative error of at most 0.0016.
Values may be sent and summed in bfloat16 or wider, within the bound.
No kernel may reach another device: no remote copies, remote signals or barrier semaphores. Data moves between devices by JAX's collectives and lax.ppermute only.
A program may use at most 128 MiB of HBM per device.

```python
import math
import jax
import jax.numpy as jnp
from jax import lax

SPECIES = 128
BLOCK = 16
LAYERS = 4
TY = 128
SUBSTEPS = 2
NBLOCK = 8
NPARAM = 16
NX = 64
NCELL = 32768


def touch_ends(values, rng, least, top_value):
    spot = [jax.random.randint(jax.random.fold_in(rng, axis), (), 0, length) for axis, length in enumerate(values.shape)]
    longest = values.shape.index(max(values.shape))
    beside = spot[:longest] + [(spot[longest] + 1) % values.shape[longest]] + spot[longest + 1:]
    return values.at[tuple(spot)].set(least).at[tuple(beside)].set(top_value)


def block_levels(key, dims, shards, smallest, largest):
    gain = 1.0
    for axis_at, blocks in shards:
        steps = jax.random.uniform(jax.random.fold_in(jax.random.fold_in(key, 6), axis_at), (blocks,), jnp.float32, smallest / len(shards), largest / len(shards))
        gain = gain * jnp.repeat(jnp.exp(steps), dims[axis_at] // blocks).reshape((-1,) + (1,) * (len(dims) - 1 - axis_at))
    return gain


def gaussian(stream_key, extent, width, bound, pieces=(), held_as=jnp.bfloat16):
    entries = width * jax.random.normal(stream_key, extent, jnp.float32)
    if pieces:
        entries = entries * block_levels(stream_key, extent, pieces, -0.22, 0.18)
    return jnp.clip(entries, -bound, bound).astype(held_as)


def setup_inputs(seed: int = 0) -> dict:
    seeds = jax.random.split(jax.random.key(seed), 11)
    return {
        "concentration": jnp.clip(jnp.exp(math.log(5.0) - 3.218876 * jax.random.uniform(seeds[0], (SPECIES, NCELL), jnp.float32) ** block_levels(seeds[0], (SPECIES, NCELL), ((1, 256),), -0.2, 0.2)), 0.2, 5.0),
        "emissions": jnp.clip(1.0 * jax.random.uniform(seeds[1], (SPECIES, NCELL), jnp.float32) ** block_levels(seeds[1], (SPECIES, NCELL), ((1, 256),), -0.2, 0.2), 0.0, 1.0),
        "rate_table": jnp.clip(jnp.exp(jax.random.uniform(seeds[2], (NBLOCK, BLOCK, BLOCK), jnp.float32, math.log(0.01), math.log(0.3))), 0.01, 0.3),
        "species_order": jax.random.permutation(seeds[3], SPECIES).astype(jnp.int32),
        "sensitivity": gaussian(seeds[4], (NPARAM, SPECIES, NX, LAYERS, TY), 1.0, 6.0, ((0, 8), (2, 32)), jnp.float32),
        "source_terms": jnp.clip(2.0 * jax.random.uniform(seeds[5], (NPARAM, SPECIES, NX, LAYERS, TY), jnp.float32) ** block_levels(seeds[5], (NPARAM, SPECIES, NX, LAYERS, TY), ((0, 8), (2, 32)), -0.2, 0.2), 0.0, 2.0).astype(jnp.bfloat16),
        "courant_x": jnp.clip(0.05 + 0.19 * jax.random.uniform(seeds[6], (NX, LAYERS, TY), jnp.float32) ** block_levels(seeds[6], (NX, LAYERS, TY), ((0, 32),), -0.2, 0.2), 0.05, 0.24),
        "upwind_x": touch_ends(jax.random.randint(seeds[7], (NX, LAYERS, TY), 0, 2), jax.random.fold_in(seeds[7], 1), 0, 1).astype(jnp.int32),
        "courant_y": jnp.clip(0.05 + 0.19 * jax.random.uniform(seeds[8], (NX, LAYERS, TY), jnp.float32) ** block_levels(seeds[8], (NX, LAYERS, TY), ((0, 32),), -0.2, 0.2), 0.05, 0.24),
        "upwind_y": touch_ends(jax.random.randint(seeds[9], (NX, LAYERS, TY), 0, 2), jax.random.fold_in(seeds[9], 1), 0, 1).astype(jnp.int32),
    }


def invert_blocks(matrix):
    size = matrix.shape[1]
    positions = jnp.arange(size)

    def eliminate(pivot_index, current):
        pivot = 1.0 / current[:, pivot_index, pivot_index, :]
        pivot_row = current[:, pivot_index, :, :] * pivot[:, None, :]
        pivot_row = jnp.where((positions == pivot_index)[None, :, None], pivot[:, None, :], pivot_row)
        column = current[:, :, pivot_index, :]
        updated = current - column[:, :, None, :] * pivot_row[:, None, :, :]
        updated = jnp.where((positions == pivot_index)[None, None, :, None], -column[:, :, None, :] * pivot[:, None, None, :], updated)
        updated = jnp.where((positions == pivot_index)[None, :, None, None], pivot_row[:, None, :, :], updated)
        return updated

    return lax.fori_loop(0, size, eliminate, matrix)


def build_factors(conc_cells, species_order, rate_table):
    block_count, block_width = rate_table.shape[0], rate_table.shape[1]
    ordered = jnp.take(conc_cells, species_order, axis=0).reshape(block_count, block_width, -1)
    coupling = rate_table[:, :, :, None] * ordered[:, None, :, :]
    row_total = jnp.sum(coupling, axis=2)
    positions = jnp.arange(block_width)
    identity = (positions[:, None] == positions[None, :]).astype(jnp.float32)
    system = identity[None, :, :, None] * (1.0 + row_total)[:, :, None, :] - coupling
    return invert_blocks(system).astype(jnp.bfloat16)


def apply_blocks(factors, values):
    result = jnp.zeros(values.shape, jnp.float32)
    for column_index in range(factors.shape[2]):
        result = result + factors[:, :, column_index, :].astype(jnp.float32)[None] * values[:, :, column_index, :][:, :, None, :]
    return result


def advect(tracer, courant_x, upwind_x, courant_y, upwind_y):
    before_x = jnp.concatenate([jnp.zeros_like(tracer[:, :, :1]), tracer[:, :, :-1]], axis=2)
    lower_x = courant_x * jnp.where(upwind_x == 1, before_x, -tracer)
    upper_x = jnp.concatenate([lower_x[:, :, 1:], jnp.zeros_like(lower_x[:, :, :1])], axis=2)
    before_y = jnp.concatenate([jnp.zeros_like(tracer[..., :1]), tracer[..., :-1]], axis=4)
    lower_y = courant_y * jnp.where(upwind_y == 1, before_y, -tracer)
    upper_y = jnp.concatenate([lower_y[..., 1:], jnp.zeros_like(lower_y[..., :1])], axis=4)
    return tracer + lower_x - upper_x + lower_y - upper_y


def reference(concentration, emissions, rate_table, species_order, sensitivity, source_terms, courant_x, upwind_x, courant_y, upwind_y):
    block_count = SPECIES // BLOCK
    plane_cells = LAYERS * TY
    tracer = sensitivity
    for substep in range(SUBSTEPS):
        tracer = advect(tracer, courant_x, upwind_x, courant_y, upwind_y)
    inverse = jnp.argsort(species_order).astype(jnp.int32)
    right_side = jnp.take(tracer + source_terms.astype(jnp.float32), species_order, axis=1)
    right_side = right_side.reshape(NPARAM, block_count, BLOCK, NX, plane_cells).transpose(3, 0, 1, 2, 4)
    base_side = jnp.take(concentration + emissions, species_order, axis=0)
    base_side = base_side.reshape(block_count, BLOCK, NX, plane_cells).transpose(2, 0, 1, 3)
    conc_planes = concentration.reshape(SPECIES, NX, plane_cells).transpose(1, 0, 2)

    def one_plane(items):
        conc_plane, base_plane, side_plane = items
        factors = build_factors(conc_plane, species_order, rate_table)
        return apply_blocks(factors, base_plane[None])[0], apply_blocks(factors, side_plane)

    new_base, new_tracer = lax.map(one_plane, (conc_planes, base_side, right_side))
    new_base = new_base.transpose(1, 2, 0, 3).reshape(SPECIES, NCELL)
    new_concentration = jnp.take(new_base, inverse, axis=0)
    new_tracer = new_tracer.transpose(1, 2, 3, 0, 4).reshape(NPARAM, SPECIES, NX, LAYERS, TY)
    new_sensitivity = jnp.take(new_tracer, inverse, axis=1)
    sensitivity_burden = jnp.sum(new_sensitivity, axis=(2, 3, 4)) / NCELL
    species_burden = jnp.sum(new_concentration, axis=1) / NCELL
    return new_concentration, new_sensitivity, sensitivity_burden, species_burden
```

```python
import functools

import jax
import jax.numpy as jnp
from jax import lax
from jax.experimental import pallas as pl
from jax.experimental.pallas import tpu as pltpu
from jax.sharding import PartitionSpec as P

ROWS, LANES = 8, 128
HIGHEST = lax.Precision.HIGHEST


def shifted(value, by, axis):
    return pltpu.roll(value, by % value.shape[axis], axis)


def coefficients(cx, ux, cy, uy, upper):
    half = ROWS // 2
    row = lax.broadcasted_iota(jnp.int32, (ROWS, LANES), 0)
    lane = lax.broadcasted_iota(jnp.int32, (ROWS, LANES), 1)
    first = row < half
    up_x = jnp.where(ux == 1, cx, 0.0)
    down_x = jnp.where(ux == 1, 0.0, cx)
    up_y = jnp.where(uy == 1, cy, 0.0)
    down_y = jnp.where(uy == 1, 0.0, cy)
    before = jnp.where(lane == 0, 0.0, up_y)
    leave = jnp.where(lane == LANES - 1, 0.0, shifted(up_y, -1, 1))
    after = jnp.where(lane == LANES - 1, 0.0, shifted(down_y, -1, 1))
    other = jnp.where(first, shifted(down_x, half, 0), up_x)
    leave_x = jnp.where(first, shifted(up_x, half, 0), upper)
    own = 1.0 - down_y - leave - down_x - leave_x
    return first, up_x, down_x, own, other, before, after


def moved(s, own, other, before, after):
    return (
        own * s
        + other * shifted(s, ROWS // 2, 0)
        + before * shifted(s, 1, 1)
        + after * shifted(s, -1, 1)
    )


def message_kernel(cx, ux, cy, uy, s_ref, right_ref, left_ref):
    half = ROWS // 2
    species = right_ref.shape[0]
    first, up_x, down_x, own, other, before, after = coefficients(
        cx[...], ux[...], cy[...], uy[...], 0.0
    )
    down = jnp.where(first, down_x, 0.0)

    def one(k, carry):
        rights, lefts = [], []
        for g in range(2):
            s = s_ref[g, k]
            t = moved(s, own, other, before, after)
            rights.append(jnp.where(first, shifted(s, half, 0), t))
            lefts.append(jnp.where(first, down * s, shifted(down * t, half, 0)))
        right_ref[k] = jnp.concatenate(rights, 0).astype(jnp.bfloat16)
        left_ref[k] = jnp.concatenate(lefts, 0).astype(jnp.bfloat16)
        return carry

    lax.fori_loop(0, species, one, 0, unroll=8)
    high = up_x.astype(jnp.bfloat16).astype(jnp.float32)
    low = up_x - high
    both = jnp.where(first, high, shifted(low, half, 0))
    left_ref[species] = jnp.concatenate([both, jnp.zeros_like(both)], 0).astype(jnp.bfloat16)


def factor_kernel(place_ref, order_ref, rate_ref, cells_ref, factor_ref, conc_ref, part_ref, m_ref, all_ref):
    n = 16
    block = pl.program_id(0)
    stride = cells_ref.shape[0] // ROWS
    species = stride // 2
    where_ = [order_ref[block * n + j] for j in range(n)]
    conc = [cells_ref[pl.ds(where_[j], ROWS, stride=stride), :] for j in range(n)]
    for i in range(n):
        total = None
        row = []
        for j in range(n):
            c = rate_ref[(block * n + i) * n + j] * conc[j]
            row.append(c)
            total = c if total is None else total + c
        for j in range(n):
            m_ref[i * n + j] = (1.0 + total) - row[j] if i == j else -row[j]

    for k in range(0, n, 2):
        x = [m_ref[k * n + j] for j in range(n)]
        y = [m_ref[(k + 1) * n + j] for j in range(n)]
        p = 1.0 / x[k]
        x = [p if j == k else x[j] * p for j in range(n)]
        e = y[k]
        y = [-(e * x[j]) if j == k else y[j] - e * x[j] for j in range(n)]
        p = 1.0 / y[k + 1]
        y = [p if j == k + 1 else y[j] * p for j in range(n)]
        e = x[k + 1]
        x = [-(e * y[j]) if j == k + 1 else x[j] - e * y[j] for j in range(n)]
        for i in range(n):
            if i in (k, k + 1):
                continue
            a = m_ref[i * n + k]
            b = m_ref[i * n + k + 1]
            for j in range(n):
                step = a * x[j] + b * y[j]
                m_ref[i * n + j] = -step if j in (k, k + 1) else m_ref[i * n + j] - step
        for j in range(n):
            m_ref[k * n + j] = x[j]
            m_ref[(k + 1) * n + j] = y[j]

    base = [
        cells_ref[pl.ds(where_[j], ROWS, stride=stride), :]
        + cells_ref[pl.ds(species + where_[j], ROWS, stride=stride), :]
        for j in range(n)
    ]
    for i in range(0, n, 2):
        sums = [None, None]
        for j in range(n):
            pair = jnp.concatenate([m_ref[i * n + j], m_ref[(i + 1) * n + j]], 0).astype(jnp.bfloat16)
            factor_ref[0, j, i // 2] = pair
            wide = pair.astype(jnp.float32)
            for h in range(2):
                term = wide[h * ROWS : (h + 1) * ROWS] * base[j]
                sums[h] = term if sums[h] is None else sums[h] + term
        for h in range(2):
            all_ref[pl.ds(pl.multiple_of(where_[i + h] * ROWS, ROWS), ROWS), :] = sums[h]

    @pl.when(block == pl.num_programs(0) - 1)
    def _():
        conc_ref[...] = all_ref[pl.ds(place_ref[0], species, stride=ROWS), :]
        rows = jnp.sum(all_ref[...].reshape(species, ROWS, LANES), axis=1)
        ones = jnp.ones((ROWS, LANES), jnp.float32)
        part_ref[...] = lax.dot_general(ones, rows, (((1,), (1,)), ((), ())), precision=HIGHEST)


def apply_kernel(
    order_ref, cx, ux, cy, uy, s_ref, source_ref, from_left_ref, from_right_ref, factor_ref, out_ref, part_ref
):
    n = 16
    half = ROWS // 2
    block = pl.program_id(0)
    species = from_left_ref.shape[0]
    extra = from_right_ref[species].astype(jnp.float32)[:ROWS]
    upper = extra + shifted(extra, half, 0)
    first, up_x, down_x, own, other, before, after = coefficients(
        cx[...], ux[...], cy[...], uy[...], upper
    )
    values = [[None] * n, [None] * n]
    for j in range(n):
        k = order_ref[block * n + j]
        left = from_left_ref[k].astype(jnp.float32)
        right = from_right_ref[k].astype(jnp.float32)
        for g in range(2):
            a = left[g * ROWS : (g + 1) * ROWS]
            b = right[g * ROWS : (g + 1) * ROWS]
            inflow = up_x * a
            halo_0 = jnp.where(first, inflow, shifted(b, half, 0))
            halo_1 = jnp.where(first, up_x * (shifted(a, half, 0) - inflow), b)
            s = s_ref[g, k]
            s = moved(s, own, other, before, after) + halo_0
            s = moved(s, own, other, before, after) + halo_1
            values[g][j] = s + source_ref[g, k].astype(jnp.float32)
    for i in range(0, n, 2):
        sums = [[None, None], [None, None]]
        for j in range(n):
            wide = factor_ref[0, j, i // 2].astype(jnp.float32)
            for h in range(2):
                f = wide[h * ROWS : (h + 1) * ROWS]
                for g in range(2):
                    term = f * values[g][j]
                    sums[g][h] = term if sums[g][h] is None else sums[g][h] + term
        for h in range(2):
            k = order_ref[block * n + i + h]
            for g in range(2):
                out_ref[g, k] = sums[g][h]

    @pl.when(block == pl.num_programs(0) - 1)
    def _():
        ones = jnp.ones((ROWS, LANES), jnp.float32)
        for g in range(2):
            rows = jnp.sum(out_ref[g], axis=1)
            part_ref[g] = lax.dot_general(ones, rows, (((1,), (1,)), ((), ())), precision=HIGHEST)


def passed_along(value, by):
    devices = lax.axis_size("cols")
    pairs = [(i, i + by) for i in range(devices) if 0 <= i + by < devices]
    return lax.ppermute(value, "cols", pairs)


VMEM = pl.BlockSpec(memory_space=pltpu.VMEM)
SMEM = pl.BlockSpec(memory_space=pltpu.SMEM)


def whole(shape):
    return pl.BlockSpec(shape, lambda b: (0,) * len(shape))


def shards(
    concentration,
    emissions,
    rate_table,
    species_order,
    sensitivity,
    source_terms,
    courant_x,
    upwind_x,
    courant_y,
    upwind_y,
):
    blocks, width = rate_table.shape[:2]
    groups, species, planes, layers, across = sensitivity.shape
    cells = planes * layers * across
    members = lax.axis_size("params")
    s = sensitivity.reshape(groups, species, ROWS, LANES)
    source = source_terms.reshape(groups, species, ROWS, LANES)
    winds = [w.reshape(ROWS, LANES) for w in (courant_x, upwind_x, courant_y, upwind_y)]

    to_right, to_left = pl.pallas_call(
        message_kernel,
        out_shape=(
            jax.ShapeDtypeStruct((species, 2 * ROWS, LANES), jnp.bfloat16),
            jax.ShapeDtypeStruct((species + 1, 2 * ROWS, LANES), jnp.bfloat16),
        ),
        in_specs=[VMEM] * 5,
        out_specs=(VMEM, VMEM),
        name="messages",
    )(*winds, s)
    from_left = passed_along(to_right, 1)
    from_right = passed_along(to_left, -1)

    both = jnp.stack([concentration, emissions])
    gathered = lax.all_gather(both, "params", axis=0).reshape(members * 2 * species, LANES)
    place = lax.axis_index("params").astype(jnp.int32).reshape(1)
    factors, new_concentration, conc_part = pl.pallas_call(
        factor_kernel,
        grid=(blocks,),
        out_shape=(
            jax.ShapeDtypeStruct((blocks, width, width // 2, 2 * ROWS, LANES), jnp.bfloat16),
            jax.ShapeDtypeStruct((species, LANES), jnp.float32),
            jax.ShapeDtypeStruct((ROWS, species), jnp.float32),
        ),
        in_specs=[SMEM, SMEM, SMEM, whole(gathered.shape)],
        out_specs=(
            pl.BlockSpec((1, width, width // 2, 2 * ROWS, LANES), lambda b: (b, 0, 0, 0, 0)),
            whole((species, LANES)),
            whole((ROWS, species)),
        ),
        scratch_shapes=[
            pltpu.VMEM((width * width, ROWS, LANES), jnp.float32),
            pltpu.VMEM((species * ROWS, LANES), jnp.float32),
        ],
        name="factors",
    )(place, species_order, rate_table.reshape(-1), gathered)

    new_sens, sens_part = pl.pallas_call(
        apply_kernel,
        grid=(blocks,),
        out_shape=(
            jax.ShapeDtypeStruct((groups, species, ROWS, LANES), jnp.float32),
            jax.ShapeDtypeStruct((groups, ROWS, species), jnp.float32),
        ),
        in_specs=[SMEM]
        + [whole((ROWS, LANES))] * 4
        + [whole(v.shape) for v in (s, source, from_left, from_right)]
        + [pl.BlockSpec((1, width, width // 2, 2 * ROWS, LANES), lambda b: (b, 0, 0, 0, 0))],
        out_specs=(whole((groups, species, ROWS, LANES)), whole((groups, ROWS, species))),
        name="apply",
    )(species_order, *winds, s, source, from_left, from_right, factors)

    parts = jnp.concatenate([sens_part[:, 0], conc_part[:1]], axis=0)
    tiles = lax.axis_size("cols")
    everything = lax.all_to_all(
        jnp.broadcast_to(parts[None], (tiles, *parts.shape)), "cols", 0, 0, tiled=True
    )
    means = jnp.sum(everything, axis=0) / (cells * tiles)
    return (
        new_concentration,
        new_sens.reshape(sensitivity.shape),
        means[:groups],
        means[groups],
    )


def solution(mesh):
    in_specs = (
        P(None, ("cols", "params")),
        P(None, ("cols", "params")),
        P(),
        P(),
        P("params", None, "cols"),
        P("params", None, "cols"),
        P("cols"),
        P("cols"),
        P("cols"),
        P("cols"),
    )
    out_specs = (P(None, ("cols", "params")), P("params", None, "cols"), P("params"), P())
    return jax.shard_map(shards, mesh=mesh, in_specs=in_specs, out_specs=out_specs, check_vma=False)
```

```python
import functools

import jax
import jax.numpy as jnp
from jax import lax
from jax.experimental import pallas as pl
from jax.experimental.pallas import tpu as pltpu
from jax.sharding import PartitionSpec as P

ROWS, LANES = 8, 128
HALF = ROWS // 2
N = 16
CHUNKS = 4
HIGHEST = lax.Precision.HIGHEST
VMEM = pl.BlockSpec(memory_space=pltpu.VMEM)
SMEM = pl.BlockSpec(memory_space=pltpu.SMEM)
ANY = pl.BlockSpec(memory_space=pl.ANY)
SMALL = pltpu.CompilerParams(vmem_limit_bytes=16 << 20)


def shifted(value, by, axis):
    return pltpu.roll(value, by % value.shape[axis], axis)


def coefficients(cx, ux, cy, uy):
    row = lax.broadcasted_iota(jnp.int32, (ROWS, LANES), 0)
    lane = lax.broadcasted_iota(jnp.int32, (ROWS, LANES), 1)
    first = row < HALF
    up_x = jnp.where(ux == 1, cx, 0.0)
    down_x = jnp.where(ux == 1, 0.0, cx)
    up_y = jnp.where(uy == 1, cy, 0.0)
    down_y = jnp.where(uy == 1, 0.0, cy)
    before = jnp.where(lane == 0, 0.0, up_y)
    leave = jnp.where(lane == LANES - 1, 0.0, shifted(up_y, -1, 1))
    after = jnp.where(lane == LANES - 1, 0.0, shifted(down_y, -1, 1))
    other = jnp.where(first, shifted(down_x, HALF, 0), up_x)
    leave_x = jnp.where(first, shifted(up_x, HALF, 0), 0.0)
    own = 1.0 - down_y - leave - down_x - leave_x
    return first, up_x, down_x, (own, other, before, after)


def moved(s, weights):
    own, other, before, after = weights
    return (
        own * s
        + other * shifted(s, HALF, 0)
        + before * shifted(s, 1, 1)
        + after * shifted(s, -1, 1)
    )


def inverted(m_ref):
    for k in range(0, N, 2):
        x = [m_ref[k * N + j] for j in range(N)]
        y = [m_ref[(k + 1) * N + j] for j in range(N)]
        p = 1.0 / x[k]
        x = [p if j == k else x[j] * p for j in range(N)]
        e = y[k]
        y = [e * -x[j] if j == k else y[j] - e * x[j] for j in range(N)]
        p = 1.0 / y[k + 1]
        y = [p if j == k + 1 else y[j] * p for j in range(N)]
        e = x[k + 1]
        x = [e * -y[j] if j == k + 1 else x[j] - e * y[j] for j in range(N)]
        minus_x = {j: -x[j] for j in (k, k + 1)}
        minus_y = {j: -y[j] for j in (k, k + 1)}
        for i in range(N):
            if i in (k, k + 1):
                continue
            a = m_ref[i * N + k]
            b = m_ref[i * N + k + 1]
            for j in range(N):
                if j in (k, k + 1):
                    m_ref[i * N + j] = a * minus_x[j] + b * minus_y[j]
                else:
                    m_ref[i * N + j] = m_ref[i * N + j] - (a * x[j] + b * y[j])
        for j in range(N):
            m_ref[k * N + j] = x[j]
            m_ref[(k + 1) * N + j] = y[j]


def minus_system(m_ref, conc, rate):
    for i in range(N):
        row = [rate(i, j) * conc[j] for j in range(N)]
        total = row[0]
        for j in range(1, N):
            total = total + row[j]
        for j in range(N):
            m_ref[i * N + j] = row[j] - (1.0 + total) if i == j else row[j]


def lane_sums(rows):
    ones = jnp.ones((ROWS, LANES), jnp.float32)
    return lax.dot_general(ones, rows, (((1,), (1,)), ((), ())), precision=HIGHEST)


def message_kernel(cx, ux, cy, uy, s_hbm, a_ref, b_ref, s_ref, weights_ref, sems):
    species = s_ref.shape[1]
    size = species // CHUNKS

    def copy(c):
        part = (slice(None), pl.ds(c * size, size))
        return pltpu.make_async_copy(s_hbm.at[part], s_ref.at[part], sems.at[c])

    for c in range(CHUNKS):
        copy(c).start()
    first, up_x, down_x, weights = coefficients(cx[...], ux[...], cy[...], uy[...])
    down = jnp.where(first, down_x, 0.0)
    for at, weight in enumerate((up_x, *weights)):
        weights_ref[at] = weight
    high = up_x.astype(jnp.bfloat16).astype(jnp.float32)
    low = up_x - high
    both = jnp.where(first, high, shifted(low, HALF, 0))
    extra = jnp.concatenate([both, jnp.zeros_like(both)], 0).astype(jnp.bfloat16)
    odd = lax.axis_index("cols") % 2 == 1

    def work(right_ref, left_ref, c):
        def one(k, carry):
            rights, lefts = [], []
            for g in range(2):
                s = s_ref[g, k]
                t = moved(s, weights)
                rights.append(jnp.where(first, shifted(s, HALF, 0), t))
                lefts.append(jnp.where(first, down * s, shifted(down * t, HALF, 0)))
            right_ref[k] = jnp.concatenate(rights, 0).astype(jnp.bfloat16)
            left_ref[k] = jnp.concatenate(lefts, 0).astype(jnp.bfloat16)
            return carry

        lax.fori_loop(c * size, (c + 1) * size, one, 0, unroll=8)

    a_ref[species] = extra
    b_ref[species] = extra
    for c in range(CHUNKS):
        copy(c).wait()

        @pl.when(odd)
        def _():
            work(a_ref, b_ref, c)

        @pl.when(jnp.logical_not(odd))
        def _():
            work(b_ref, a_ref, c)


def base_kernel(order_ref, rate_ref, conc_ref, emis_ref, packet_ref, new_ref, m_ref, c_ref, e_ref, r_ref):
    species = conc_ref.shape[0]
    blocks = species // N
    for b in range(blocks):
        for j in range(N):
            k = order_ref[b * N + j]
            c_ref[pl.ds(j * ROWS + b, 1), :] = conc_ref[pl.ds(k, 1), :]
            e_ref[pl.ds(j * ROWS + b, 1), :] = emis_ref[pl.ds(k, 1), :]
    conc = [c_ref[pl.ds(j * ROWS, ROWS), :] for j in range(N)]

    for b in range(blocks):
        for i in range(N):
            r_ref[pl.ds(i * ROWS + b, 1), :] = rate_ref[b, pl.ds(i, 1), :]

    def rate(i, j):
        return jnp.broadcast_to(r_ref[pl.ds(i * ROWS, ROWS), j : j + 1], (ROWS, LANES))

    minus_system(m_ref, conc, rate)
    inverted(m_ref)
    values = [
        -(c_ref[pl.ds(j * ROWS, ROWS), :] + e_ref[pl.ds(j * ROWS, ROWS), :]) for j in range(N)
    ]
    for i in range(N):
        total = None
        for j in range(N):
            term = m_ref[i * N + j].astype(jnp.bfloat16).astype(jnp.float32) * values[j]
            total = term if total is None else total + term
        e_ref[pl.ds(i * ROWS, ROWS), :] = total
    for b in range(blocks):
        for i in range(N):
            k = order_ref[b * N + i]
            new_ref[pl.ds(k, 1), :] = e_ref[pl.ds(i * ROWS + b, 1), :]
    packet_ref[:species, :] = conc_ref[...]
    packet_ref[species:, :] = lane_sums(new_ref[...])


def factor_kernel(order_ref, rate_ref, cells_ref, source_hbm, factor_ref, part_ref, source_ref, m_ref, sem):
    stride = cells_ref.shape[0] // ROWS
    species = stride - ROWS
    blocks = species // N
    copy = pltpu.make_async_copy(source_hbm, source_ref, sem)
    copy.start()

    def one(block, carry):
        conc = [
            cells_ref[pl.ds(order_ref[block * N + j], ROWS, stride=stride), :] for j in range(N)
        ]
        minus_system(m_ref, conc, lambda i, j: rate_ref[block, i, j])
        inverted(m_ref)
        for i in range(0, N, 2):
            for j in range(N):
                pair = jnp.concatenate([m_ref[i * N + j], m_ref[(i + 1) * N + j]], 0)
                factor_ref[block, j, i // 2] = pair.astype(jnp.bfloat16)
        return carry

    lax.fori_loop(0, blocks, one, 0)
    members = cells_ref[pl.ds(species, ROWS, stride=stride), :]
    part_ref[...] = jnp.sum(members, axis=0, keepdims=True)
    copy.wait()


def apply_kernel(
    order_ref, weights_ref, s_ref, source_ref, a_ref, b_ref, factor_ref, conc_part_ref, out_ref, part_ref
):
    species = s_ref.shape[1]
    odd = lax.axis_index("cols") % 2 == 1
    extra = jnp.where(odd, a_ref[species].astype(jnp.float32), b_ref[species].astype(jnp.float32))
    extra = extra[:ROWS]
    upper = extra + shifted(extra, HALF, 0)
    first = lax.broadcasted_iota(jnp.int32, (ROWS, LANES), 0) < HALF
    up_x = weights_ref[0]
    own = weights_ref[1] - jnp.where(first, 0.0, upper)
    weights = (own, weights_ref[2], weights_ref[3], weights_ref[4])
    minus = tuple(-w for w in weights)

    def one(block, carry):
        values = [[None] * N, [None] * N]
        for j in range(N):
            k = order_ref[block * N + j]
            wide_a = a_ref[k].astype(jnp.float32)
            wide_b = b_ref[k].astype(jnp.float32)
            left = jnp.where(odd, wide_b, wide_a)
            right = jnp.where(odd, wide_a, wide_b)
            for g in range(2):
                a = left[g * ROWS : (g + 1) * ROWS]
                b = right[g * ROWS : (g + 1) * ROWS]
                inflow = up_x * a
                halo_0 = jnp.where(first, inflow, shifted(b, HALF, 0))
                halo_1 = jnp.where(first, up_x * (shifted(a, HALF, 0) - inflow), b)
                s = moved(s_ref[g, k], weights) + halo_0
                s = moved(s, minus) - halo_1
                values[g][j] = s - source_ref[g, k].astype(jnp.float32)
        for i in range(0, N, 2):
            sums = [[None, None], [None, None]]
            for j in range(N):
                wide = factor_ref[block, j, i // 2].astype(jnp.float32)
                for h in range(2):
                    f = wide[h * ROWS : (h + 1) * ROWS]
                    for g in range(2):
                        term = f * values[g][j]
                        sums[g][h] = term if sums[g][h] is None else sums[g][h] + term
            for h in range(2):
                k = order_ref[block * N + i + h]
                for g in range(2):
                    out_ref[g, k] = sums[g][h]
        return carry

    lax.fori_loop(0, species // N, one, 0)
    tiles = part_ref.shape[0]
    for g in range(2):
        row = lane_sums(jnp.sum(out_ref[g], axis=1))[:1]
        part_ref[:, g, :] = jnp.broadcast_to(row, (tiles, LANES))
    part_ref[:, 2, :] = jnp.broadcast_to(conc_part_ref[...], (tiles, LANES))


def means_kernel(scale, parts_ref, sens_ref, conc_ref):
    totals = jnp.sum(parts_ref[...], axis=0) * scale
    sens_ref[...] = totals[:2]
    conc_ref[...] = totals[2:3]


def near(value):
    return pltpu.with_memory_space_constraint(value, pltpu.VMEM)


def far(value):
    return pltpu.with_memory_space_constraint(value, pltpu.HBM)


def swapped(value, first):
    devices = lax.axis_size("cols")
    pairs = [(i, i + 1) for i in range(first, devices - 1, 2)]
    return lax.ppermute(value, "cols", pairs + [(b, a) for a, b in pairs])


def shards(
    concentration,
    emissions,
    rate_table,
    species_order,
    sensitivity,
    source_terms,
    courant_x,
    upwind_x,
    courant_y,
    upwind_y,
):
    blocks = rate_table.shape[0]
    groups, species, planes, layers, across = sensitivity.shape
    cells = planes * layers * across
    tiles = lax.axis_size("cols")
    s = sensitivity.reshape(groups, species, ROWS, LANES)
    source = source_terms.reshape(groups, species, ROWS, LANES)
    winds = [w.reshape(ROWS, LANES) for w in (courant_x, upwind_x, courant_y, upwind_y)]

    message = pltpu.VMEM((species + 1, 2 * ROWS, LANES), jnp.bfloat16)
    a, b, s_near, weights = pl.pallas_call(
        message_kernel,
        out_shape=(
            message,
            message,
            pltpu.VMEM(s.shape, jnp.float32),
            pltpu.VMEM((5, ROWS, LANES), jnp.float32),
        ),
        in_specs=[VMEM] * 4 + [ANY],
        out_specs=(VMEM,) * 4,
        scratch_shapes=[pltpu.SemaphoreType.DMA((CHUNKS,))],
        compiler_params=SMALL,
        name="messages",
    )(*map(far, winds), far(s))
    a = swapped(a, 1)
    b = swapped(b, 0)

    packet, new_concentration = pl.pallas_call(
        base_kernel,
        out_shape=(
            pltpu.VMEM((species + ROWS, LANES), jnp.float32),
            jax.ShapeDtypeStruct((species, LANES), jnp.float32),
        ),
        in_specs=[SMEM, VMEM, VMEM, VMEM],
        out_specs=(VMEM, VMEM),
        scratch_shapes=[
            pltpu.VMEM((N * N, ROWS, LANES), jnp.float32),
            pltpu.VMEM((species, LANES), jnp.float32),
            pltpu.VMEM((species, LANES), jnp.float32),
            pltpu.VMEM((N * ROWS, N), jnp.float32),
        ],
        compiler_params=SMALL,
        name="base",
    )(far(species_order), far(rate_table), far(concentration), far(emissions))
    gathered = lax.all_gather(packet, "params", axis=0, tiled=True)

    factors, conc_part, source_near = pl.pallas_call(
        factor_kernel,
        out_shape=(
            pltpu.VMEM((blocks, N, N // 2, 2 * ROWS, LANES), jnp.bfloat16),
            pltpu.VMEM((1, LANES), jnp.float32),
            pltpu.VMEM(source.shape, source.dtype),
        ),
        in_specs=[SMEM, SMEM, VMEM, ANY],
        out_specs=(VMEM,) * 3,
        scratch_shapes=[
            pltpu.VMEM((N * N, ROWS, LANES), jnp.float32),
            pltpu.SemaphoreType.DMA,
        ],
        compiler_params=SMALL,
        name="factors",
    )(far(species_order), far(rate_table), near(gathered), far(source))

    new_sens, parts = pl.pallas_call(
        apply_kernel,
        out_shape=(
            pltpu.VMEM(s.shape, jnp.float32),
            pltpu.VMEM((tiles, 3, LANES), jnp.float32),
        ),
        in_specs=[SMEM] + [VMEM] * 7,
        out_specs=(VMEM, VMEM),
        compiler_params=SMALL,
        name="apply",
    )(
        far(species_order),
        near(weights),
        near(s_near),
        near(source_near),
        near(a),
        near(b),
        near(factors),
        near(conc_part),
    )

    everything = lax.all_to_all(parts, "cols", 0, 0, tiled=True)
    sens_mean, conc_mean = pl.pallas_call(
        functools.partial(means_kernel, 1.0 / (cells * tiles)),
        out_shape=(
            jax.ShapeDtypeStruct((groups, species), jnp.float32),
            jax.ShapeDtypeStruct((1, species), jnp.float32),
        ),
        in_specs=[VMEM],
        out_specs=(VMEM, VMEM),
        compiler_params=SMALL,
        name="means",
    )(near(everything))
    return (
        new_concentration,
        new_sens.reshape(sensitivity.shape),
        sens_mean,
        conc_mean.reshape(species),
    )


def solution(mesh):
    in_specs = (
        P(None, ("cols", "params")),
        P(None, ("cols", "params")),
        P(),
        P(),
        P("params", None, "cols"),
        P("params", None, "cols"),
        P("cols"),
        P("cols"),
        P("cols"),
        P("cols"),
    )
    out_specs = (P(None, ("cols", "params")), P("params", None, "cols"), P("params"), P())
    return jax.shard_map(shards, mesh=mesh, in_specs=in_specs, out_specs=out_specs, check_vma=False)
```

```python
import functools

import jax
import jax.numpy as jnp
from jax import lax
from jax.experimental import pallas as pl
from jax.experimental.pallas import tpu as pltpu
from jax.sharding import PartitionSpec as P


ROWS, LANES = 8, 128
HALF = ROWS // 2
N = 16
CHUNKS = 4
HIGHEST = lax.Precision.HIGHEST
VMEM = pl.BlockSpec(memory_space=pltpu.VMEM)
SMEM = pl.BlockSpec(memory_space=pltpu.SMEM)
ANY = pl.BlockSpec(memory_space=pl.ANY)
SMALL = pltpu.CompilerParams(vmem_limit_bytes=16 << 20)


def shifted(value, by, axis):
    return pltpu.roll(value, by % value.shape[axis], axis)


def coefficients(cx, ux, cy, uy):
    row = lax.broadcasted_iota(jnp.int32, (ROWS, LANES), 0)
    lane = lax.broadcasted_iota(jnp.int32, (ROWS, LANES), 1)
    first = row < HALF
    up_x = jnp.where(ux == 1, cx, 0.0)
    down_x = jnp.where(ux == 1, 0.0, cx)
    up_y = jnp.where(uy == 1, cy, 0.0)
    down_y = jnp.where(uy == 1, 0.0, cy)
    before = jnp.where(lane == 0, 0.0, up_y)
    leave = jnp.where(lane == LANES - 1, 0.0, shifted(up_y, -1, 1))
    after = jnp.where(lane == LANES - 1, 0.0, shifted(down_y, -1, 1))
    other = jnp.where(first, shifted(down_x, HALF, 0), up_x)
    leave_x = jnp.where(first, shifted(up_x, HALF, 0), 0.0)
    own = 1.0 - down_y - leave - down_x - leave_x
    return first, up_x, down_x, (own, other, before, after)


def moved(s, weights):
    own, other, before, after = weights
    return (
        own * s
        + other * shifted(s, HALF, 0)
        + before * shifted(s, 1, 1)
        + after * shifted(s, -1, 1)
    )


def inverted(m_ref):
    for k in range(0, N, 2):
        x = [m_ref[k * N + j] for j in range(N)]
        y = [m_ref[(k + 1) * N + j] for j in range(N)]
        p = 1.0 / x[k]
        x = [p if j == k else x[j] * p for j in range(N)]
        e = y[k]
        y = [e * -x[j] if j == k else y[j] - e * x[j] for j in range(N)]
        p = 1.0 / y[k + 1]
        y = [p if j == k + 1 else y[j] * p for j in range(N)]
        e = x[k + 1]
        x = [e * -y[j] if j == k + 1 else x[j] - e * y[j] for j in range(N)]
        minus_x = {j: -x[j] for j in (k, k + 1)}
        minus_y = {j: -y[j] for j in (k, k + 1)}
        for i in range(N):
            if i in (k, k + 1):
                continue
            a = m_ref[i * N + k]
            b = m_ref[i * N + k + 1]
            for j in range(N):
                if j in (k, k + 1):
                    m_ref[i * N + j] = a * minus_x[j] + b * minus_y[j]
                else:
                    m_ref[i * N + j] = m_ref[i * N + j] - (a * x[j] + b * y[j])
        for j in range(N):
            m_ref[k * N + j] = x[j]
            m_ref[(k + 1) * N + j] = y[j]


def minus_system(m_ref, conc, rate):
    for i in range(N):
        row = [rate(i, j) * conc[j] for j in range(N)]
        total = row[0]
        for j in range(1, N):
            total = total + row[j]
        for j in range(N):
            m_ref[i * N + j] = row[j] - (1.0 + total) if i == j else row[j]


def lane_sums(rows):
    ones = jnp.ones((ROWS, LANES), jnp.float32)
    return lax.dot_general(ones, rows, (((1,), (1,)), ((), ())), precision=HIGHEST)


def message_kernel(cx, ux, cy, uy, s_hbm, a_ref, b_ref, s_ref, weights_ref, sems):
    species = s_ref.shape[1]
    size = species // CHUNKS

    def copy(c):
        part = (slice(None), pl.ds(c * size, size))
        return pltpu.make_async_copy(s_hbm.at[part], s_ref.at[part], sems.at[c])

    for c in range(CHUNKS):
        copy(c).start()
    first, up_x, down_x, weights = coefficients(cx[...], ux[...], cy[...], uy[...])
    down = jnp.where(first, down_x, 0.0)
    for at, weight in enumerate((up_x, *weights)):
        weights_ref[at] = weight
    high = up_x.astype(jnp.bfloat16).astype(jnp.float32)
    low = up_x - high
    both = jnp.where(first, high, shifted(low, HALF, 0))
    extra = jnp.concatenate([both, jnp.zeros_like(both)], 0).astype(jnp.bfloat16)
    odd = lax.axis_index("cols") % 2 == 1

    def work(right_ref, left_ref, c):
        def one(k, carry):
            rights, lefts = [], []
            for g in range(2):
                s = s_ref[g, k]
                t = moved(s, weights)
                rights.append(jnp.where(first, shifted(s, HALF, 0), t))
                lefts.append(jnp.where(first, down * s, shifted(down * t, HALF, 0)))
            right_ref[k] = jnp.concatenate(rights, 0).astype(jnp.bfloat16)
            left_ref[k] = jnp.concatenate(lefts, 0).astype(jnp.bfloat16)
            return carry

        lax.fori_loop(c * size, (c + 1) * size, one, 0, unroll=8)

    a_ref[species] = extra
    b_ref[species] = extra
    for c in range(CHUNKS):
        copy(c).wait()

        @pl.when(odd)
        def _():
            work(a_ref, b_ref, c)

        @pl.when(jnp.logical_not(odd))
        def _():
            work(b_ref, a_ref, c)


def base_kernel(order_ref, rate_ref, conc_ref, emis_ref, part_ref, new_ref, m_ref, c_ref, e_ref, r_ref):
    species = conc_ref.shape[0]
    blocks = species // N
    for b in range(blocks):
        for j in range(N):
            k = order_ref[b * N + j]
            c_ref[pl.ds(j * ROWS + b, 1), :] = conc_ref[pl.ds(k, 1), :]
            e_ref[pl.ds(j * ROWS + b, 1), :] = emis_ref[pl.ds(k, 1), :]
    conc = [c_ref[pl.ds(j * ROWS, ROWS), :] for j in range(N)]

    for b in range(blocks):
        for i in range(N):
            r_ref[pl.ds(i * ROWS + b, 1), :] = rate_ref[b, pl.ds(i, 1), :]

    def rate(i, j):
        return jnp.broadcast_to(r_ref[pl.ds(i * ROWS, ROWS), j : j + 1], (ROWS, LANES))

    minus_system(m_ref, conc, rate)
    inverted(m_ref)
    values = [
        -(c_ref[pl.ds(j * ROWS, ROWS), :] + e_ref[pl.ds(j * ROWS, ROWS), :]) for j in range(N)
    ]
    for i in range(N):
        total = None
        for j in range(N):
            term = m_ref[i * N + j].astype(jnp.bfloat16).astype(jnp.float32) * values[j]
            total = term if total is None else total + term
        e_ref[pl.ds(i * ROWS, ROWS), :] = total
    for b in range(blocks):
        for i in range(N):
            k = order_ref[b * N + i]
            new_ref[pl.ds(k, 1), :] = e_ref[pl.ds(i * ROWS + b, 1), :]
    part_ref[...] = lane_sums(new_ref[...])


def factor_kernel(
    order_ref, rate_ref, mine_ref, other_ref, source_hbm, factor_ref, source_ref, cells_ref, m_ref, sem
):
    links, species = mine_ref.shape[:2]
    blocks = species // N
    copy = pltpu.make_async_copy(source_hbm, source_ref, sem)
    copy.start()
    place = lax.axis_index("params")
    for k in range(links):
        for core, ref in enumerate((mine_ref, other_ref)):
            cells_ref[pl.ds(place ^ (2 * k + core), species, stride=ROWS), :] = ref[k]

    def one(block, carry):
        conc = [
            cells_ref[pl.ds(pl.multiple_of(order_ref[block * N + j] * ROWS, ROWS), ROWS), :]
            for j in range(N)
        ]
        minus_system(m_ref, conc, lambda i, j: rate_ref[block, i, j])
        inverted(m_ref)
        for i in range(0, N, 2):
            for j in range(N):
                pair = jnp.concatenate([m_ref[i * N + j], m_ref[(i + 1) * N + j]], 0)
                factor_ref[block, j, i // 2] = pair.astype(jnp.bfloat16)
        return carry

    lax.fori_loop(0, blocks, one, 0)
    copy.wait()


def apply_kernel(
    order_ref, weights_ref, s_ref, source_ref, a_ref, b_ref, factor_ref, conc_part_ref, out_ref, part_ref
):
    species = s_ref.shape[1]
    odd = lax.axis_index("cols") % 2 == 1
    extra = jnp.where(odd, a_ref[species].astype(jnp.float32), b_ref[species].astype(jnp.float32))
    extra = extra[:ROWS]
    upper = extra + shifted(extra, HALF, 0)
    first = lax.broadcasted_iota(jnp.int32, (ROWS, LANES), 0) < HALF
    up_x = weights_ref[0]
    own = weights_ref[1] - jnp.where(first, 0.0, upper)
    weights = (own, weights_ref[2], weights_ref[3], weights_ref[4])
    minus = tuple(-w for w in weights)

    def one(block, carry):
        values = [[None] * N, [None] * N]
        for j in range(N):
            k = order_ref[block * N + j]
            wide_a = a_ref[k].astype(jnp.float32)
            wide_b = b_ref[k].astype(jnp.float32)
            left = jnp.where(odd, wide_b, wide_a)
            right = jnp.where(odd, wide_a, wide_b)
            for g in range(2):
                a = left[g * ROWS : (g + 1) * ROWS]
                b = right[g * ROWS : (g + 1) * ROWS]
                inflow = up_x * a
                halo_0 = jnp.where(first, inflow, shifted(b, HALF, 0))
                halo_1 = jnp.where(first, up_x * (shifted(a, HALF, 0) - inflow), b)
                s = moved(s_ref[g, k], weights) + halo_0
                s = moved(s, minus) - halo_1
                values[g][j] = s - source_ref[g, k].astype(jnp.float32)
        for i in range(0, N, 2):
            sums = [[None, None], [None, None]]
            for j in range(N):
                wide = factor_ref[block, j, i // 2].astype(jnp.float32)
                for h in range(2):
                    f = wide[h * ROWS : (h + 1) * ROWS]
                    for g in range(2):
                        term = f * values[g][j]
                        sums[g][h] = term if sums[g][h] is None else sums[g][h] + term
            for h in range(2):
                k = order_ref[block * N + i + h]
                for g in range(2):
                    out_ref[g, k] = sums[g][h]
        return carry

    lax.fori_loop(0, species // N, one, 0)
    tiles = part_ref.shape[0]
    for g in range(2):
        row = lane_sums(jnp.sum(out_ref[g], axis=1))[:1]
        part_ref[:, g, :] = jnp.broadcast_to(row, (tiles, LANES))
    part_ref[:, 2, :] = jnp.broadcast_to(conc_part_ref[:1], (tiles, LANES))


def means_kernel(scale, parts_ref, sens_ref, conc_ref):
    totals = jnp.sum(parts_ref[...], axis=0) * scale
    sens_ref[...] = totals[:2]
    conc_ref[...] = totals[2:3]


def near(value):
    return pltpu.with_memory_space_constraint(value, pltpu.VMEM)


def far(value):
    return pltpu.with_memory_space_constraint(value, pltpu.HBM)


def crossed(value, bits):
    return lax.ppermute(
        value, "params", [(i, i ^ bits) for i in range(lax.axis_size("params"))]
    )


def swapped(value, first):
    devices = lax.axis_size("cols")
    pairs = [(i, i + 1) for i in range(first, devices - 1, 2)]
    return lax.ppermute(value, "cols", pairs + [(b, a) for a, b in pairs])


def step(
    concentration,
    emissions,
    rate_table,
    species_order,
    sensitivity,
    source_terms,
    courant_x,
    upwind_x,
    courant_y,
    upwind_y,
):
    blocks = rate_table.shape[0]
    groups, species, planes, layers, across = sensitivity.shape
    cells = planes * layers * across
    tiles = lax.axis_size("cols")
    s = sensitivity.reshape(groups, species, ROWS, LANES)
    source = source_terms.reshape(groups, species, ROWS, LANES)
    winds = [w.reshape(ROWS, LANES) for w in (courant_x, upwind_x, courant_y, upwind_y)]

    links = lax.axis_size("params") // 2
    mine = [concentration]
    for k in range(1, links):
        mine.append(crossed(concentration, 2 * k))
    message = pltpu.VMEM((species + 1, 2 * ROWS, LANES), jnp.bfloat16)
    a, b, s_near, weights = pl.pallas_call(
        message_kernel,
        out_shape=(
            message,
            message,
            pltpu.VMEM(s.shape, jnp.float32),
            pltpu.VMEM((5, ROWS, LANES), jnp.float32),
        ),
        in_specs=[VMEM] * 4 + [ANY],
        out_specs=(VMEM,) * 4,
        scratch_shapes=[pltpu.SemaphoreType.DMA((CHUNKS,))],
        compiler_params=SMALL,
        name="messages",
    )(*map(far, winds), far(s))
    a = swapped(a, 1)
    b = swapped(b, 0)
    mine = jnp.stack(mine)
    other = crossed(mine, 1)

    conc_part, new_concentration = pl.pallas_call(
        base_kernel,
        out_shape=(
            pltpu.VMEM((ROWS, LANES), jnp.float32),
            jax.ShapeDtypeStruct((species, LANES), jnp.float32),
        ),
        in_specs=[SMEM, VMEM, VMEM, VMEM],
        out_specs=(VMEM, VMEM),
        scratch_shapes=[
            pltpu.VMEM((N * N, ROWS, LANES), jnp.float32),
            pltpu.VMEM((species, LANES), jnp.float32),
            pltpu.VMEM((species, LANES), jnp.float32),
            pltpu.VMEM((N * ROWS, N), jnp.float32),
        ],
        compiler_params=SMALL,
        name="base",
    )(far(species_order), far(rate_table), far(concentration), far(emissions))
    conc_part = conc_part + crossed(conc_part, 1)
    others = []
    for k in range(1, links):
        others.append(crossed(conc_part, 2 * k))
    conc_part = sum(others, conc_part)

    factors, source_near = pl.pallas_call(
        factor_kernel,
        out_shape=(
            pltpu.VMEM((blocks, N, N // 2, 2 * ROWS, LANES), jnp.bfloat16),
            pltpu.VMEM(source.shape, source.dtype),
        ),
        in_specs=[SMEM, SMEM, VMEM, VMEM, ANY],
        out_specs=(VMEM,) * 2,
        scratch_shapes=[
            pltpu.VMEM((species * ROWS, LANES), jnp.float32),
            pltpu.VMEM((N * N, ROWS, LANES), jnp.float32),
            pltpu.SemaphoreType.DMA,
        ],
        compiler_params=SMALL,
        name="factors",
    )(far(species_order), far(rate_table), near(mine), near(other), far(source))

    new_sens, parts = pl.pallas_call(
        apply_kernel,
        out_shape=(
            pltpu.VMEM(s.shape, jnp.float32),
            pltpu.VMEM((tiles, 3, LANES), jnp.float32),
        ),
        in_specs=[SMEM] + [VMEM] * 7,
        out_specs=(VMEM, VMEM),
        compiler_params=SMALL,
        name="apply",
    )(
        far(species_order),
        near(weights),
        near(s_near),
        near(source_near),
        near(a),
        near(b),
        near(factors),
        near(conc_part),
    )

    everything = lax.all_to_all(parts, "cols", 0, 0, tiled=True)
    sens_mean, conc_mean = pl.pallas_call(
        functools.partial(means_kernel, 1.0 / (cells * tiles)),
        out_shape=(
            jax.ShapeDtypeStruct((groups, species), jnp.float32),
            jax.ShapeDtypeStruct((1, species), jnp.float32),
        ),
        in_specs=[VMEM],
        out_specs=(VMEM, VMEM),
        compiler_params=SMALL,
        name="means",
    )(near(everything))
    return (
        new_concentration,
        new_sens.reshape(sensitivity.shape),
        sens_mean,
        conc_mean.reshape(species),
    )


def solution(mesh):
    in_specs = (
        P(None, ("cols", "params")),
        P(None, ("cols", "params")),
        P(),
        P(),
        P("params", None, "cols"),
        P("params", None, "cols"),
        P("cols"),
        P("cols"),
        P("cols"),
        P("cols"),
    )
    out_specs = (P(None, ("cols", "params")), P("params", None, "cols"), P("params"), P())
    return jax.shard_map(step, mesh=mesh, in_specs=in_specs, out_specs=out_specs, check_vma=False)
```

```python
import functools

import jax
import jax.numpy as jnp
from jax import lax
from jax.experimental import pallas as pl
from jax.experimental.pallas import tpu as pltpu
from jax.sharding import PartitionSpec as P


ROWS, LANES = 8, 128
HALF = ROWS // 2
N = 16
CHUNKS = 8
HIGHEST = lax.Precision.HIGHEST
VMEM = pl.BlockSpec(memory_space=pltpu.VMEM)
SMEM = pl.BlockSpec(memory_space=pltpu.SMEM)
ANY = pl.BlockSpec(memory_space=pl.ANY)
SMALL = pltpu.CompilerParams(vmem_limit_bytes=16 << 20)


def shifted(value, by, axis):
    return pltpu.roll(value, by % value.shape[axis], axis)


def coefficients(cx, ux, cy, uy):
    row = lax.broadcasted_iota(jnp.int32, (ROWS, LANES), 0)
    lane = lax.broadcasted_iota(jnp.int32, (ROWS, LANES), 1)
    first = row < HALF
    up_x = jnp.where(ux == 1, cx, 0.0)
    down_x = jnp.where(ux == 1, 0.0, cx)
    up_y = jnp.where(uy == 1, cy, 0.0)
    down_y = jnp.where(uy == 1, 0.0, cy)
    before = jnp.where(lane == 0, 0.0, up_y)
    leave = jnp.where(lane == LANES - 1, 0.0, shifted(up_y, -1, 1))
    after = jnp.where(lane == LANES - 1, 0.0, shifted(down_y, -1, 1))
    other = jnp.where(first, shifted(down_x, HALF, 0), up_x)
    leave_x = jnp.where(first, shifted(up_x, HALF, 0), 0.0)
    own = 1.0 - down_y - leave - down_x - leave_x
    return first, up_x, down_x, (own, other, before, after)


def moved(s, weights):
    own, other, before, after = weights
    return (
        own * s
        + other * shifted(s, HALF, 0)
        + before * shifted(s, 1, 1)
        + after * shifted(s, -1, 1)
    )


def inverted(m_ref):
    for k in range(0, N, 2):
        x = [m_ref[k * N + j] for j in range(N)]
        y = [m_ref[(k + 1) * N + j] for j in range(N)]
        p = 1.0 / x[k]
        x = [p if j == k else x[j] * p for j in range(N)]
        e = y[k]
        y = [e * -x[j] if j == k else y[j] - e * x[j] for j in range(N)]
        p = 1.0 / y[k + 1]
        y = [p if j == k + 1 else y[j] * p for j in range(N)]
        e = x[k + 1]
        x = [e * -y[j] if j == k + 1 else x[j] - e * y[j] for j in range(N)]
        minus_x = {j: -x[j] for j in (k, k + 1)}
        minus_y = {j: -y[j] for j in (k, k + 1)}
        for i in range(N):
            if i in (k, k + 1):
                continue
            a = m_ref[i * N + k]
            b = m_ref[i * N + k + 1]
            for j in range(N):
                if j in (k, k + 1):
                    m_ref[i * N + j] = a * minus_x[j] + b * minus_y[j]
                else:
                    m_ref[i * N + j] = m_ref[i * N + j] - (a * x[j] + b * y[j])
        for j in range(N):
            m_ref[k * N + j] = x[j]
            m_ref[(k + 1) * N + j] = y[j]


def minus_system(m_ref, conc, rate):
    for i in range(N):
        row = [rate(i, j) * conc[j] for j in range(N)]
        total = row[0]
        for j in range(1, N):
            total = total + row[j]
        for j in range(N):
            m_ref[i * N + j] = row[j] - (1.0 + total) if i == j else row[j]


def lane_sums(rows):
    ones = jnp.ones((ROWS, LANES), jnp.float32)
    return lax.dot_general(ones, rows, (((1,), (1,)), ((), ())), precision=HIGHEST)


def message_kernel(
    cx_hbm, ux_hbm, cy_hbm, uy_hbm, s_hbm, a_ref, b_ref, s_ref, t_ref, weights_ref, reals_ref, flags_ref, wind_sem, sems
):
    species = s_ref.shape[1]
    size = species // CHUNKS

    def copy(c):
        part = (slice(None), pl.ds(c * size, size))
        return pltpu.make_async_copy(s_hbm.at[part], s_ref.at[part], sems.at[c])

    winds = [
        pltpu.make_async_copy(source, target, wind_sem.at[at])
        for at, (source, target) in enumerate(
            (
                (cx_hbm, reals_ref.at[0]),
                (ux_hbm, flags_ref.at[0]),
                (cy_hbm, reals_ref.at[1]),
                (uy_hbm, flags_ref.at[1]),
            )
        )
    ]
    for wind in winds:
        wind.start()
    for c in range(CHUNKS):
        copy(c).start()
    for wind in winds:
        wind.wait()
    first, up_x, down_x, weights = coefficients(
        reals_ref[0], flags_ref[0], reals_ref[1], flags_ref[1]
    )
    down = jnp.where(first, down_x, 0.0)
    for at, weight in enumerate((up_x, *weights)):
        weights_ref[at] = weight
    high = up_x.astype(jnp.bfloat16).astype(jnp.float32)
    low = up_x - high
    both = jnp.where(first, high, shifted(low, HALF, 0))
    extra = jnp.concatenate([both, jnp.zeros_like(both)], 0).astype(jnp.bfloat16)
    odd = lax.axis_index("cols") % 2 == 1
    a_ref[species] = extra
    b_ref[species] = extra

    def work(right_ref, left_ref):
        def chunk(c, carry):
            copy(c).wait()
            for at in range(size):
                k = c * size + at
                rights, lefts = [], []
                for g in range(2):
                    s = s_ref[g, k]
                    t = moved(s, weights)
                    t_ref[g, k] = t
                    rights.append(jnp.where(first, shifted(s, HALF, 0), t))
                    lefts.append(jnp.where(first, down * s, shifted(down * t, HALF, 0)))
                right_ref[k] = jnp.concatenate(rights, 0).astype(jnp.bfloat16)
                left_ref[k] = jnp.concatenate(lefts, 0).astype(jnp.bfloat16)
            return carry

        lax.fori_loop(0, CHUNKS, chunk, 0)

    @pl.when(odd)
    def _():
        work(a_ref, b_ref)

    @pl.when(jnp.logical_not(odd))
    def _():
        work(b_ref, a_ref)


def base_kernel(order_ref, rate_ref, conc_ref, emis_ref, part_ref, new_ref, m_ref, c_ref, e_ref, r_ref):
    species = conc_ref.shape[0]
    blocks = species // N
    for b in range(blocks):
        for j in range(N):
            k = order_ref[b * N + j]
            c_ref[pl.ds(j * ROWS + b, 1), :] = conc_ref[pl.ds(k, 1), :]
            e_ref[pl.ds(j * ROWS + b, 1), :] = emis_ref[pl.ds(k, 1), :]
    conc = [c_ref[pl.ds(j * ROWS, ROWS), :] for j in range(N)]

    for b in range(blocks):
        for i in range(N):
            r_ref[pl.ds(i * ROWS + b, 1), :] = rate_ref[b, pl.ds(i, 1), :]

    def rate(i, j):
        return jnp.broadcast_to(r_ref[pl.ds(i * ROWS, ROWS), j : j + 1], (ROWS, LANES))

    minus_system(m_ref, conc, rate)
    inverted(m_ref)
    values = [
        -(c_ref[pl.ds(j * ROWS, ROWS), :] + e_ref[pl.ds(j * ROWS, ROWS), :]) for j in range(N)
    ]
    for i in range(N):
        total = None
        for j in range(N):
            term = m_ref[i * N + j].astype(jnp.bfloat16).astype(jnp.float32) * values[j]
            total = term if total is None else total + term
        e_ref[pl.ds(i * ROWS, ROWS), :] = total
    for b in range(blocks):
        for i in range(N):
            k = order_ref[b * N + i]
            new_ref[pl.ds(k, 1), :] = e_ref[pl.ds(i * ROWS + b, 1), :]
    part_ref[...] = lane_sums(new_ref[...])


def factor_kernel(
    order_ref, rate_ref, mine_ref, other_ref, source_hbm, factor_ref, source_ref, cells_ref, m_ref, sem
):
    links, species = mine_ref.shape[:2]
    blocks = species // N
    copy = pltpu.make_async_copy(source_hbm, source_ref, sem)
    copy.start()
    place = lax.axis_index("params")
    for k in range(links):
        for core, ref in enumerate((mine_ref, other_ref)):
            cells_ref[pl.ds(place ^ (2 * k + core), species, stride=ROWS), :] = ref[k]

    def one(block, carry):
        conc = [
            cells_ref[pl.ds(pl.multiple_of(order_ref[block * N + j] * ROWS, ROWS), ROWS), :]
            for j in range(N)
        ]
        minus_system(m_ref, conc, lambda i, j: rate_ref[block, i, j])
        inverted(m_ref)
        for i in range(0, N, 2):
            for j in range(N):
                pair = jnp.concatenate([m_ref[i * N + j], m_ref[(i + 1) * N + j]], 0)
                factor_ref[block, j, i // 2] = pair.astype(jnp.bfloat16).astype(jnp.float32)
        return carry

    lax.fori_loop(0, blocks, one, 0)
    copy.wait()


def apply_kernel(
    order_ref,
    weights_ref,
    s_ref,
    t_ref,
    source_ref,
    a_ref,
    b_ref,
    factor_ref,
    conc_part_ref,
    out_ref,
    part_ref,
    even_ref,
    odd_ref,
):
    species = s_ref.shape[1]
    blocks = species // N
    odd = lax.axis_index("cols") % 2 == 1
    extra = jnp.where(odd, a_ref[species].astype(jnp.float32), b_ref[species].astype(jnp.float32))
    extra = extra[:ROWS]
    first = lax.broadcasted_iota(jnp.int32, (ROWS, LANES), 0) < HALF
    upper = jnp.where(first, 0.0, extra + shifted(extra, HALF, 0))
    up_x = weights_ref[0]
    minus = (upper - weights_ref[1],) + tuple(-weights_ref[at] for at in range(2, 5))

    def values(block, j, ref):
        k = order_ref[block * N + j]
        wide_a = a_ref[k].astype(jnp.float32)
        wide_b = b_ref[k].astype(jnp.float32)
        left = jnp.where(odd, wide_b, wide_a)
        right = jnp.where(odd, wide_a, wide_b)
        for g in range(2):
            a = left[g * ROWS : (g + 1) * ROWS]
            b = right[g * ROWS : (g + 1) * ROWS]
            inflow = up_x * a
            halo_0 = jnp.where(first, inflow, shifted(b, HALF, 0))
            halo_1 = jnp.where(first, up_x * (shifted(a, HALF, 0) - inflow), b)
            s = (t_ref[g, k] - upper * s_ref[g, k]) + halo_0
            s = moved(s, minus) - halo_1
            ref[j * 2 + g] = s - source_ref[g, k].astype(jnp.float32)

    def products(block, i, ref):
        sums = [[None, None], [None, None]]
        for j in range(N):
            wide = factor_ref[block, j, i]
            for h in range(2):
                f = wide[h * ROWS : (h + 1) * ROWS]
                for g in range(2):
                    term = f * ref[j * 2 + g]
                    sums[g][h] = term if sums[g][h] is None else sums[g][h] + term
        for h in range(2):
            k = order_ref[block * N + 2 * i + h]
            for g in range(2):
                out_ref[g, k] = sums[g][h]

    for j in range(N):
        values(0, j, even_ref)

    def two(pair, carry):
        block = 2 * pair
        for now, later, ref, other in (
            (block, block + 1, even_ref, odd_ref),
            (block + 1, lax.rem(block + 2, blocks), odd_ref, even_ref),
        ):
            for i in range(N // 2):
                products(now, i, ref)
                values(later, 2 * i, other)
                values(later, 2 * i + 1, other)
        return carry

    lax.fori_loop(0, blocks // 2, two, 0)
    tiles = part_ref.shape[0]
    for g in range(2):
        row = lane_sums(jnp.sum(out_ref[g], axis=1))[:1]
        part_ref[:, g, :] = jnp.broadcast_to(row, (tiles, LANES))
    part_ref[:, 2, :] = jnp.broadcast_to(conc_part_ref[:1], (tiles, LANES))


def means_kernel(scale, parts_ref, sens_ref, conc_ref):
    totals = jnp.sum(parts_ref[...], axis=0) * scale
    sens_ref[...] = totals[:2]
    conc_ref[...] = totals[2:3]


def near(value):
    return pltpu.with_memory_space_constraint(value, pltpu.VMEM)


def far(value):
    return pltpu.with_memory_space_constraint(value, pltpu.HBM)


def crossed(value, bits):
    return lax.ppermute(
        value, "params", [(i, i ^ bits) for i in range(lax.axis_size("params"))]
    )


def swapped(value, first):
    devices = lax.axis_size("cols")
    pairs = [(i, i + 1) for i in range(first, devices - 1, 2)]
    return lax.ppermute(value, "cols", pairs + [(b, a) for a, b in pairs])


def step(
    concentration,
    emissions,
    rate_table,
    species_order,
    sensitivity,
    source_terms,
    courant_x,
    upwind_x,
    courant_y,
    upwind_y,
):
    blocks = rate_table.shape[0]
    groups, species, planes, layers, across = sensitivity.shape
    cells = planes * layers * across
    tiles = lax.axis_size("cols")
    s = sensitivity.reshape(groups, species, ROWS, LANES)
    source = source_terms.reshape(groups, species, ROWS, LANES)
    winds = [w.reshape(ROWS, LANES) for w in (courant_x, upwind_x, courant_y, upwind_y)]

    links = lax.axis_size("params") // 2
    mine = [concentration]
    for k in range(1, links):
        mine.append(crossed(concentration, 2 * k))
    message = pltpu.VMEM((species + 1, 2 * ROWS, LANES), jnp.bfloat16)
    a, b, s_near, t_near, weights = pl.pallas_call(
        message_kernel,
        out_shape=(
            message,
            message,
            pltpu.VMEM(s.shape, jnp.float32),
            pltpu.VMEM(s.shape, jnp.float32),
            pltpu.VMEM((5, ROWS, LANES), jnp.float32),
        ),
        in_specs=[ANY] * 5,
        out_specs=(VMEM,) * 5,
        scratch_shapes=[
            pltpu.VMEM((2, ROWS, LANES), jnp.float32),
            pltpu.VMEM((2, ROWS, LANES), jnp.int32),
            pltpu.SemaphoreType.DMA((4,)),
            pltpu.SemaphoreType.DMA((CHUNKS,)),
        ],
        compiler_params=SMALL,
        name="messages",
    )(*map(far, winds), far(s))
    a = swapped(a, 1)
    b = swapped(b, 0)
    mine = jnp.stack(mine)
    other = crossed(mine, 1)

    conc_part, new_concentration = pl.pallas_call(
        base_kernel,
        out_shape=(
            pltpu.VMEM((ROWS, LANES), jnp.float32),
            jax.ShapeDtypeStruct((species, LANES), jnp.float32),
        ),
        in_specs=[SMEM, VMEM, VMEM, VMEM],
        out_specs=(VMEM, VMEM),
        scratch_shapes=[
            pltpu.VMEM((N * N, ROWS, LANES), jnp.float32),
            pltpu.VMEM((species, LANES), jnp.float32),
            pltpu.VMEM((species, LANES), jnp.float32),
            pltpu.VMEM((N * ROWS, N), jnp.float32),
        ],
        compiler_params=SMALL,
        name="base",
    )(far(species_order), far(rate_table), far(concentration), far(emissions))
    conc_part = conc_part + crossed(conc_part, 1)
    others = []
    for k in range(1, links):
        others.append(crossed(conc_part, 2 * k))
    conc_part = sum(others, conc_part)

    factors, source_near = pl.pallas_call(
        factor_kernel,
        out_shape=(
            pltpu.VMEM((blocks, N, N // 2, 2 * ROWS, LANES), jnp.float32),
            pltpu.VMEM(source.shape, source.dtype),
        ),
        in_specs=[SMEM, SMEM, VMEM, VMEM, ANY],
        out_specs=(VMEM,) * 2,
        scratch_shapes=[
            pltpu.VMEM((species * ROWS, LANES), jnp.float32),
            pltpu.VMEM((N * N, ROWS, LANES), jnp.float32),
            pltpu.SemaphoreType.DMA,
        ],
        compiler_params=SMALL,
        name="factors",
    )(far(species_order), far(rate_table), near(mine), near(other), far(source))

    new_sens, parts = pl.pallas_call(
        apply_kernel,
        out_shape=(
            pltpu.VMEM(s.shape, jnp.float32),
            pltpu.VMEM((tiles, 3, LANES), jnp.float32),
        ),
        in_specs=[SMEM] + [VMEM] * 8,
        out_specs=(VMEM, VMEM),
        scratch_shapes=[pltpu.VMEM((2 * N, ROWS, LANES), jnp.float32)] * 2,
        compiler_params=SMALL,
        name="apply",
    )(
        far(species_order),
        near(weights),
        near(s_near),
        near(t_near),
        near(source_near),
        near(a),
        near(b),
        near(factors),
        near(conc_part),
    )

    everything = lax.all_to_all(parts, "cols", 0, 0, tiled=True)
    sens_mean, conc_mean = pl.pallas_call(
        functools.partial(means_kernel, 1.0 / (cells * tiles)),
        out_shape=(
            jax.ShapeDtypeStruct((groups, species), jnp.float32),
            jax.ShapeDtypeStruct((1, species), jnp.float32),
        ),
        in_specs=[VMEM],
        out_specs=(VMEM, VMEM),
        compiler_params=SMALL,
        name="means",
    )(near(everything))
    return (
        new_concentration,
        new_sens.reshape(sensitivity.shape),
        sens_mean,
        conc_mean.reshape(species),
    )


def solution(mesh):
    in_specs = (
        P(None, ("cols", "params")),
        P(None, ("cols", "params")),
        P(),
        P(),
        P("params", None, "cols"),
        P("params", None, "cols"),
        P("cols"),
        P("cols"),
        P("cols"),
        P("cols"),
    )
    out_specs = (P(None, ("cols", "params")), P("params", None, "cols"), P("params"), P())
    return jax.shard_map(step, mesh=mesh, in_specs=in_specs, out_specs=out_specs, check_vma=False)
```

```python
import functools
import math

import jax
import jax.numpy as jnp
from jax import lax
from jax.experimental import pallas as pl
from jax.experimental.pallas import tpu as pltpu
from jax.sharding import PartitionSpec as P


ROWS, LANES = 8, 128
HALF = ROWS // 2
N = 16
CHUNKS = 8
RUN = 4
LEAST, SPAN = 0.2, math.log(25.0)
TOP, CENTRE = 65535.0, 32768.0
HIGHEST = lax.Precision.HIGHEST
VMEM = pl.BlockSpec(memory_space=pltpu.VMEM)
SMEM = pl.BlockSpec(memory_space=pltpu.SMEM)
ANY = pl.BlockSpec(memory_space=pl.ANY)
SMALL = pltpu.CompilerParams(vmem_limit_bytes=16 << 20)


def shifted(value, by, axis):
    return pltpu.roll(value, by % value.shape[axis], axis)


def coefficients(cx, ux, cy, uy):
    row = lax.broadcasted_iota(jnp.int32, (ROWS, LANES), 0)
    lane = lax.broadcasted_iota(jnp.int32, (ROWS, LANES), 1)
    first = row < HALF
    up_x = jnp.where(ux == 1, cx, 0.0)
    down_x = jnp.where(ux == 1, 0.0, cx)
    up_y = jnp.where(uy == 1, cy, 0.0)
    down_y = jnp.where(uy == 1, 0.0, cy)
    before = jnp.where(lane == 0, 0.0, up_y)
    leave = jnp.where(lane == LANES - 1, 0.0, shifted(up_y, -1, 1))
    after = jnp.where(lane == LANES - 1, 0.0, shifted(down_y, -1, 1))
    other = jnp.where(first, shifted(down_x, HALF, 0), up_x)
    leave_x = jnp.where(first, shifted(up_x, HALF, 0), 0.0)
    own = 1.0 - down_y - leave - down_x - leave_x
    return first, up_x, down_x, (own, other, before, after)


def moved(s, weights):
    own, other, before, after = weights
    return (
        own * s
        + other * shifted(s, HALF, 0)
        + before * shifted(s, 1, 1)
        + after * shifted(s, -1, 1)
    )


def inverted(m_ref):
    for k in range(0, N, 2):
        x = [m_ref[k * N + j] for j in range(N)]
        y = [m_ref[(k + 1) * N + j] for j in range(N)]
        p = 1.0 / x[k]
        x = [p if j == k else x[j] * p for j in range(N)]
        e = y[k]
        y = [e * -x[j] if j == k else y[j] - e * x[j] for j in range(N)]
        p = 1.0 / y[k + 1]
        y = [p if j == k + 1 else y[j] * p for j in range(N)]
        e = x[k + 1]
        x = [e * -y[j] if j == k + 1 else x[j] - e * y[j] for j in range(N)]
        minus_x = {j: -x[j] for j in (k, k + 1)}
        minus_y = {j: -y[j] for j in (k, k + 1)}
        for i in range(N):
            if i in (k, k + 1):
                continue
            a = m_ref[i * N + k]
            b = m_ref[i * N + k + 1]
            for j in range(N):
                if j in (k, k + 1):
                    m_ref[i * N + j] = a * minus_x[j] + b * minus_y[j]
                else:
                    m_ref[i * N + j] = m_ref[i * N + j] - (a * x[j] + b * y[j])
        for j in range(N):
            m_ref[k * N + j] = x[j]
            m_ref[(k + 1) * N + j] = y[j]


def minus_system(m_ref, conc, rate):
    for i in range(N):
        row = [rate(i, j) * conc[j] for j in range(N)]
        total = row[0]
        for j in range(1, N):
            total = total + row[j]
        for j in range(N):
            m_ref[i * N + j] = row[j] - (1.0 + total) if i == j else row[j]


def lane_sums(rows):
    ones = jnp.ones((ROWS, LANES), jnp.float32)
    return lax.dot_general(ones, rows, (((1,), (1,)), ((), ())), precision=HIGHEST)


def coded(unit):
    steps = jnp.clip(jnp.floor(unit * TOP + 0.5), 0.0, TOP) - CENTRE
    return steps.astype(jnp.int32).astype(jnp.int16)


def decoded(code):
    return (code.astype(jnp.int32).astype(jnp.float32) + CENTRE) * (1.0 / TOP)


def packet_kernel(conc_ref, emis_ref, packet_ref):
    packet_ref[0] = coded(jnp.log(conc_ref[...] * (1.0 / LEAST)) * (1.0 / SPAN))
    packet_ref[1] = coded(emis_ref[...])


def message_kernel(
    cx_hbm,
    ux_hbm,
    cy_hbm,
    uy_hbm,
    s_hbm,
    a_ref,
    b_ref,
    half_0_ref,
    half_1_ref,
    s_ref,
    t_ref,
    weights_ref,
    reals_ref,
    flags_ref,
    wind_sem,
    sems,
):
    species = s_ref.shape[1]
    size = species // CHUNKS

    def copy(c):
        part = (slice(None), pl.ds(c * size, size))
        return pltpu.make_async_copy(s_hbm.at[part], s_ref.at[part], sems.at[c])

    winds = [
        pltpu.make_async_copy(source, target, wind_sem.at[at])
        for at, (source, target) in enumerate(
            (
                (cx_hbm, reals_ref.at[0]),
                (ux_hbm, flags_ref.at[0]),
                (cy_hbm, reals_ref.at[1]),
                (uy_hbm, flags_ref.at[1]),
            )
        )
    ]
    for wind in winds:
        wind.start()
    for c in range(CHUNKS):
        copy(c).start()
    for wind in winds:
        wind.wait()
    first, up_x, down_x, weights = coefficients(
        reals_ref[0], flags_ref[0], reals_ref[1], flags_ref[1]
    )
    down = jnp.where(first, down_x, 0.0)
    for at, weight in enumerate((up_x, *weights)):
        weights_ref[at] = weight
    high = up_x.astype(jnp.bfloat16).astype(jnp.float32)
    low = up_x - high
    both = jnp.where(first, high, shifted(low, HALF, 0))
    extra = jnp.concatenate([both, jnp.zeros_like(both)], 0).astype(jnp.bfloat16)
    odd = lax.axis_index("cols") % 2 == 1
    a_ref[species] = extra
    b_ref[species] = extra
    half_0_ref[species] = extra[:ROWS]

    def work(right_ref, left_ref, to_right):
        def chunk(c, carry):
            copy(c).wait()
            for at in range(size):
                k = c * size + at
                rights, lefts = [], []
                for g in range(2):
                    s = s_ref[g, k]
                    t = moved(s, weights)
                    t_ref[g, k] = t
                    rights.append(jnp.where(first, shifted(s, HALF, 0), t))
                    lefts.append(jnp.where(first, down * s, shifted(down * t, HALF, 0)))
                right_ref[k] = jnp.concatenate(rights, 0).astype(jnp.bfloat16)
                left_ref[k] = jnp.concatenate(lefts, 0).astype(jnp.bfloat16)
                halves = rights if to_right else lefts
                half_0_ref[k] = halves[0].astype(jnp.bfloat16)
                half_1_ref[k] = halves[1].astype(jnp.bfloat16)
            return carry

        lax.fori_loop(0, CHUNKS, chunk, 0)

    @pl.when(odd)
    def _():
        work(a_ref, b_ref, True)

    @pl.when(jnp.logical_not(odd))
    def _():
        work(b_ref, a_ref, False)


def factor_kernel(
    order_ref,
    rate_ref,
    mine_ref,
    other_ref,
    conc_ref,
    emis_ref,
    source_hbm,
    factor_ref,
    new_ref,
    part_ref,
    source_ref,
    cells_ref,
    added_ref,
    all_ref,
    m_ref,
    sem,
):
    links, _, species = mine_ref.shape[:3]
    blocks = species // N
    copy = pltpu.make_async_copy(source_hbm, source_ref, sem)
    copy.start()
    place = lax.axis_index("params")
    for k in range(links):
        for core, ref in enumerate((mine_ref, other_ref)):
            rows = pl.ds(place ^ (2 * k + core), species, stride=ROWS)
            if k == 0 and core == 0:
                cells_ref[rows, :] = conc_ref[...]
                added_ref[rows, :] = emis_ref[...]
            else:
                cells_ref[rows, :] = LEAST * jnp.exp(SPAN * decoded(ref[k, 0]))
                added_ref[rows, :] = decoded(ref[k, 1])

    def one(block, carry):
        tiles = [
            pl.ds(pl.multiple_of(order_ref[block * N + j] * ROWS, ROWS), ROWS) for j in range(N)
        ]
        conc = [cells_ref[tile, :] for tile in tiles]
        minus_system(m_ref, conc, lambda i, j: rate_ref[block, i, j])
        inverted(m_ref)
        values = [-(cells_ref[tile, :] + added_ref[tile, :]) for tile in tiles]
        for i in range(0, N, 2):
            sums = [None, None]
            for j in range(N):
                pair = jnp.concatenate([m_ref[i * N + j], m_ref[(i + 1) * N + j]], 0)
                wide = pair.astype(jnp.bfloat16).astype(jnp.float32)
                factor_ref[block, j, i // 2] = wide
                for h in range(2):
                    term = wide[h * ROWS : (h + 1) * ROWS] * values[j]
                    sums[h] = term if sums[h] is None else sums[h] + term
            for h in range(2):
                all_ref[tiles[i + h], :] = sums[h]
        return carry

    lax.fori_loop(0, blocks, one, 0)
    new_ref[...] = all_ref[pl.ds(place, species, stride=ROWS), :]
    part_ref[...] = lane_sums(jnp.sum(all_ref[...].reshape(species, ROWS, LANES), axis=1))
    copy.wait()


def apply_kernel(
    order_ref,
    weights_ref,
    s_ref,
    t_ref,
    source_ref,
    a_ref,
    b_ref,
    half_0_ref,
    half_1_ref,
    factor_ref,
    conc_part_ref,
    out_ref,
    part_ref,
    even_ref,
    odd_ref,
):
    species = s_ref.shape[1]
    blocks = species // N
    tile = lax.axis_index("cols")
    odd = tile % 2 == 1
    relayed = is_late(tile) & ((tile % RUN == 0) | (tile % RUN == RUN - 1))
    extra_a = jnp.where(
        relayed,
        half_0_ref[species].astype(jnp.float32),
        a_ref[species].astype(jnp.float32)[:ROWS],
    )
    extra = jnp.where(odd, extra_a, b_ref[species].astype(jnp.float32)[:ROWS])
    first = lax.broadcasted_iota(jnp.int32, (ROWS, LANES), 0) < HALF
    upper = jnp.where(first, 0.0, extra + shifted(extra, HALF, 0))
    up_x = weights_ref[0]
    minus = (upper - weights_ref[1],) + tuple(-weights_ref[at] for at in range(2, 5))

    def values(block, j, ref):
        k = order_ref[block * N + j]
        wide_a = a_ref[k].astype(jnp.float32)
        wide_b = b_ref[k].astype(jnp.float32)
        for g, half_ref in enumerate((half_0_ref, half_1_ref)):
            from_a = jnp.where(
                relayed, half_ref[k].astype(jnp.float32), wide_a[g * ROWS : (g + 1) * ROWS]
            )
            from_b = wide_b[g * ROWS : (g + 1) * ROWS]
            a = jnp.where(odd, from_b, from_a)
            b = jnp.where(odd, from_a, from_b)
            inflow = up_x * a
            halo_0 = jnp.where(first, inflow, shifted(b, HALF, 0))
            halo_1 = jnp.where(first, up_x * (shifted(a, HALF, 0) - inflow), b)
            s = (t_ref[g, k] - upper * s_ref[g, k]) + halo_0
            s = moved(s, minus) - halo_1
            ref[j * 2 + g] = s - source_ref[g, k].astype(jnp.float32)

    def products(block, i, ref):
        sums = [[None, None], [None, None]]
        for j in range(N):
            wide = factor_ref[block, j, i]
            for h in range(2):
                f = wide[h * ROWS : (h + 1) * ROWS]
                for g in range(2):
                    term = f * ref[j * 2 + g]
                    sums[g][h] = term if sums[g][h] is None else sums[g][h] + term
        for h in range(2):
            k = order_ref[block * N + 2 * i + h]
            for g in range(2):
                out_ref[g, k] = sums[g][h]

    for j in range(N):
        values(0, j, even_ref)

    def two(pair, carry):
        block = 2 * pair
        for now, later, ref, other in (
            (block, block + 1, even_ref, odd_ref),
            (block + 1, lax.rem(block + 2, blocks), odd_ref, even_ref),
        ):
            for i in range(N // 2):
                products(now, i, ref)
                values(later, 2 * i, other)
                values(later, 2 * i + 1, other)
        return carry

    lax.fori_loop(0, blocks // 2, two, 0)
    tiles = part_ref.shape[0]
    for g in range(2):
        row = lane_sums(jnp.sum(out_ref[g], axis=1))[:1]
        part_ref[:, g, :] = jnp.broadcast_to(row, (tiles, LANES))
    part_ref[:, 2, :] = jnp.broadcast_to(conc_part_ref[:1], (tiles, LANES))


def means_kernel(scale, parts_ref, sens_ref, conc_ref):
    totals = jnp.sum(parts_ref[...], axis=0) * scale
    sens_ref[...] = totals[:2]
    conc_ref[...] = totals[2:3]


def near(value):
    return pltpu.with_memory_space_constraint(value, pltpu.VMEM)


def far(value):
    return pltpu.with_memory_space_constraint(value, pltpu.HBM)


def crossed(value, bits):
    return lax.ppermute(
        value, "params", [(i, i ^ bits) for i in range(lax.axis_size("params"))]
    )


def is_late(tile):
    return (tile // RUN) % 2 == 1


def edges(first):
    pairs = [(i, i + 1) for i in range(first, lax.axis_size("cols") - 1, 2)]
    return pairs + [(b, a) for a, b in pairs]


def leaps():
    return [
        (a, a - 1 if a < b else a + 1, b)
        for a, b in edges(1)
        if a // RUN != b // RUN and not is_late(a)
    ]


def passed(value, pairs):
    return lax.ppermute(value, "cols", pairs)


def step(
    concentration,
    emissions,
    rate_table,
    species_order,
    sensitivity,
    source_terms,
    courant_x,
    upwind_x,
    courant_y,
    upwind_y,
):
    blocks = rate_table.shape[0]
    groups, species, planes, layers, across = sensitivity.shape
    cells = planes * layers * across
    tiles = lax.axis_size("cols")
    s = sensitivity.reshape(groups, species, ROWS, LANES)
    source = source_terms.reshape(groups, species, ROWS, LANES)
    winds = [w.reshape(ROWS, LANES) for w in (courant_x, upwind_x, courant_y, upwind_y)]

    links = lax.axis_size("params") // 2
    message = pltpu.VMEM((species + 1, 2 * ROWS, LANES), jnp.bfloat16)
    packet = pl.pallas_call(
        packet_kernel,
        out_shape=pltpu.VMEM((2, species, LANES), jnp.int16),
        in_specs=[VMEM, VMEM],
        out_specs=VMEM,
        compiler_params=SMALL,
        name="packet",
    )(far(concentration), far(emissions))
    mine = [packet]
    for k in range(1, links):
        mine.append(crossed(packet, 2 * k))
    a, b, half_0, half_1, s_near, t_near, weights = pl.pallas_call(
        message_kernel,
        out_shape=(
            message,
            message,
            pltpu.VMEM((species + 1, ROWS, LANES), jnp.bfloat16),
            pltpu.VMEM((species, ROWS, LANES), jnp.bfloat16),
            pltpu.VMEM(s.shape, jnp.float32),
            pltpu.VMEM(s.shape, jnp.float32),
            pltpu.VMEM((5, ROWS, LANES), jnp.float32),
        ),
        in_specs=[ANY] * 5,
        out_specs=(VMEM,) * 7,
        scratch_shapes=[
            pltpu.VMEM((2, ROWS, LANES), jnp.float32),
            pltpu.VMEM((2, ROWS, LANES), jnp.int32),
            pltpu.SemaphoreType.DMA((4,)),
            pltpu.SemaphoreType.DMA((CHUNKS,)),
        ],
        compiler_params=SMALL,
        name="messages",
    )(*map(far, winds), far(s))
    far_edges = leaps()
    direct = [(u, v) for u, _, v in far_edges]
    a = passed(a, [edge for edge in edges(1) if edge not in direct])
    half_1 = passed(half_1, [(u, w) for u, w, _ in far_edges])
    half_0 = passed(half_0, direct)
    half_1 = passed(half_1, [(w, v) for _, w, v in far_edges])
    b = passed(b, edges(0))
    mine = jnp.stack(mine)
    other = crossed(mine, 1)

    factors, new_concentration, conc_part, source_near = pl.pallas_call(
        factor_kernel,
        out_shape=(
            pltpu.VMEM((blocks, N, N // 2, 2 * ROWS, LANES), jnp.float32),
            jax.ShapeDtypeStruct((species, LANES), jnp.float32),
            pltpu.VMEM((ROWS, LANES), jnp.float32),
            pltpu.VMEM(source.shape, source.dtype),
        ),
        in_specs=[SMEM, SMEM, VMEM, VMEM, VMEM, VMEM, ANY],
        out_specs=(VMEM,) * 4,
        scratch_shapes=[
            pltpu.VMEM((species * ROWS, LANES), jnp.float32),
            pltpu.VMEM((species * ROWS, LANES), jnp.float32),
            pltpu.VMEM((species * ROWS, LANES), jnp.float32),
            pltpu.VMEM((N * N, ROWS, LANES), jnp.float32),
            pltpu.SemaphoreType.DMA,
        ],
        compiler_params=SMALL,
        name="factors",
    )(
        far(species_order),
        far(rate_table),
        near(mine),
        near(other),
        far(concentration),
        far(emissions),
        far(source),
    )

    new_sens, parts = pl.pallas_call(
        apply_kernel,
        out_shape=(
            pltpu.VMEM(s.shape, jnp.float32),
            pltpu.VMEM((tiles, 3, LANES), jnp.float32),
        ),
        in_specs=[SMEM] + [VMEM] * 10,
        out_specs=(VMEM, VMEM),
        scratch_shapes=[pltpu.VMEM((2 * N, ROWS, LANES), jnp.float32)] * 2,
        compiler_params=SMALL,
        name="apply",
    )(
        far(species_order),
        near(weights),
        near(s_near),
        near(t_near),
        near(source_near),
        near(a),
        near(b),
        near(half_0),
        near(half_1),
        near(factors),
        near(conc_part),
    )

    everything = lax.all_to_all(parts, "cols", 0, 0, tiled=True)
    sens_mean, conc_mean = pl.pallas_call(
        functools.partial(means_kernel, 1.0 / (cells * tiles)),
        out_shape=(
            jax.ShapeDtypeStruct((groups, species), jnp.float32),
            jax.ShapeDtypeStruct((1, species), jnp.float32),
        ),
        in_specs=[VMEM],
        out_specs=(VMEM, VMEM),
        compiler_params=SMALL,
        name="means",
    )(near(everything))
    return (
        new_concentration,
        new_sens.reshape(sensitivity.shape),
        sens_mean,
        conc_mean.reshape(species),
    )


def solution(mesh):
    in_specs = (
        P(None, ("cols", "params")),
        P(None, ("cols", "params")),
        P(),
        P(),
        P("params", None, "cols"),
        P("params", None, "cols"),
        P("cols"),
        P("cols"),
        P("cols"),
        P("cols"),
    )
    out_specs = (P(None, ("cols", "params")), P("params", None, "cols"), P("params"), P())
    return jax.shard_map(step, mesh=mesh, in_specs=in_specs, out_specs=out_specs, check_vma=False)
```

```python
import functools
import math

import jax
import jax.numpy as jnp
from jax import lax
from jax.experimental import pallas as pl
from jax.experimental.pallas import tpu as pltpu
from jax.sharding import PartitionSpec as P


ROWS, LANES = 8, 128
HALF = ROWS // 2
N = 16
CHUNKS = 8
RUN = 4
LEAST, SPAN = 0.2, math.log(25.0)
TOP, CENTRE = 65535.0, 32768.0
HIGHEST = lax.Precision.HIGHEST
VMEM = pl.BlockSpec(memory_space=pltpu.VMEM)
SMEM = pl.BlockSpec(memory_space=pltpu.SMEM)
ANY = pl.BlockSpec(memory_space=pl.ANY)
SMALL = pltpu.CompilerParams(vmem_limit_bytes=16 << 20)


def shifted(value, by, axis):
    return pltpu.roll(value, by % value.shape[axis], axis)


def coefficients(cx, ux, cy, uy):
    row = lax.broadcasted_iota(jnp.int32, (ROWS, LANES), 0)
    lane = lax.broadcasted_iota(jnp.int32, (ROWS, LANES), 1)
    first = row < HALF
    up_x = jnp.where(ux == 1, cx, 0.0)
    down_x = jnp.where(ux == 1, 0.0, cx)
    up_y = jnp.where(uy == 1, cy, 0.0)
    down_y = jnp.where(uy == 1, 0.0, cy)
    before = jnp.where(lane == 0, 0.0, up_y)
    leave = jnp.where(lane == LANES - 1, 0.0, shifted(up_y, -1, 1))
    after = jnp.where(lane == LANES - 1, 0.0, shifted(down_y, -1, 1))
    other = jnp.where(first, shifted(down_x, HALF, 0), up_x)
    leave_x = jnp.where(first, shifted(up_x, HALF, 0), 0.0)
    own = 1.0 - down_y - leave - down_x - leave_x
    return first, up_x, down_x, (own, other, before, after)


def moved(s, weights):
    own, other, before, after = weights
    return (
        own * s
        + other * shifted(s, HALF, 0)
        + before * shifted(s, 1, 1)
        + after * shifted(s, -1, 1)
    )


def inverted(m_ref):
    for k in range(0, N, 2):
        x = [m_ref[k * N + j] for j in range(N)]
        y = [m_ref[(k + 1) * N + j] for j in range(N)]
        p = 1.0 / x[k]
        x = [p if j == k else x[j] * p for j in range(N)]
        e = y[k]
        y = [e * -x[j] if j == k else y[j] - e * x[j] for j in range(N)]
        p = 1.0 / y[k + 1]
        y = [p if j == k + 1 else y[j] * p for j in range(N)]
        e = x[k + 1]
        x = [e * -y[j] if j == k + 1 else x[j] - e * y[j] for j in range(N)]
        minus_x = {j: -x[j] for j in (k, k + 1)}
        minus_y = {j: -y[j] for j in (k, k + 1)}
        for i in range(N):
            if i in (k, k + 1):
                continue
            a = m_ref[i * N + k]
            b = m_ref[i * N + k + 1]
            for j in range(N):
                if j in (k, k + 1):
                    m_ref[i * N + j] = a * minus_x[j] + b * minus_y[j]
                else:
                    m_ref[i * N + j] = m_ref[i * N + j] - (a * x[j] + b * y[j])
        for j in range(N):
            m_ref[k * N + j] = x[j]
            m_ref[(k + 1) * N + j] = y[j]


def minus_system(m_ref, conc, rate):
    for i in range(N):
        row = [rate(i, j) * conc[j] for j in range(N)]
        total = row[0]
        for j in range(1, N):
            total = total + row[j]
        for j in range(N):
            m_ref[i * N + j] = row[j] - (1.0 + total) if i == j else row[j]


def lane_sums(rows):
    ones = jnp.ones((ROWS, LANES), jnp.float32)
    return lax.dot_general(ones, rows, (((1,), (1,)), ((), ())), precision=HIGHEST)


def coded(unit):
    steps = jnp.clip(jnp.floor(unit * TOP + 0.5), 0.0, TOP) - CENTRE
    return steps.astype(jnp.int32).astype(jnp.int16)


def decoded(code):
    return (code.astype(jnp.int32).astype(jnp.float32) + CENTRE) * (1.0 / TOP)


def packet_kernel(conc_ref, emis_ref, packet_ref):
    packet_ref[0] = coded(jnp.log(conc_ref[...] * (1.0 / LEAST)) * (1.0 / SPAN))
    packet_ref[1] = coded(emis_ref[...])


def message_kernel(
    cx_hbm,
    ux_hbm,
    cy_hbm,
    uy_hbm,
    s_hbm,
    a_ref,
    b_ref,
    half_0_ref,
    half_1_ref,
    s_ref,
    t_ref,
    weights_ref,
    reals_ref,
    flags_ref,
    wind_sem,
    sems,
):
    species = s_ref.shape[1]
    size = species // CHUNKS

    def copy(c):
        part = (slice(None), pl.ds(c * size, size))
        return pltpu.make_async_copy(s_hbm.at[part], s_ref.at[part], sems.at[c])

    winds = [
        pltpu.make_async_copy(source, target, wind_sem.at[at])
        for at, (source, target) in enumerate(
            (
                (cx_hbm, reals_ref.at[0]),
                (ux_hbm, flags_ref.at[0]),
                (cy_hbm, reals_ref.at[1]),
                (uy_hbm, flags_ref.at[1]),
            )
        )
    ]
    for wind in winds:
        wind.start()
    for c in range(CHUNKS):
        copy(c).start()
    for wind in winds:
        wind.wait()
    first, up_x, down_x, weights = coefficients(
        reals_ref[0], flags_ref[0], reals_ref[1], flags_ref[1]
    )
    down = jnp.where(first, down_x, 0.0)
    for at, weight in enumerate((up_x, *weights)):
        weights_ref[at] = weight
    high = up_x.astype(jnp.bfloat16).astype(jnp.float32)
    low = up_x - high
    both = jnp.where(first, high, shifted(low, HALF, 0))
    extra = jnp.concatenate([both, jnp.zeros_like(both)], 0).astype(jnp.bfloat16)
    odd = lax.axis_index("cols") % 2 == 1
    a_ref[species] = extra
    b_ref[species] = extra
    half_0_ref[species] = extra[:ROWS]

    def work(right_ref, left_ref, to_right):
        def chunk(c, carry):
            copy(c).wait()
            for at in range(size):
                k = c * size + at
                rights, lefts = [], []
                for g in range(2):
                    s = s_ref[g, k]
                    t = moved(s, weights)
                    t_ref[g, k] = t
                    rights.append(jnp.where(first, shifted(s, HALF, 0), t))
                    lefts.append(jnp.where(first, down * s, shifted(down * t, HALF, 0)))
                right_ref[k] = jnp.concatenate(rights, 0).astype(jnp.bfloat16)
                left_ref[k] = jnp.concatenate(lefts, 0).astype(jnp.bfloat16)
                halves = rights if to_right else lefts
                half_0_ref[k] = halves[0].astype(jnp.bfloat16)
                half_1_ref[k] = halves[1].astype(jnp.bfloat16)
            return carry

        lax.fori_loop(0, CHUNKS, chunk, 0)

    @pl.when(odd)
    def _():
        work(a_ref, b_ref, True)

    @pl.when(jnp.logical_not(odd))
    def _():
        work(b_ref, a_ref, False)


def factor_kernel(
    order_ref,
    rate_ref,
    mine_ref,
    other_ref,
    conc_ref,
    emis_ref,
    source_hbm,
    factor_ref,
    new_ref,
    part_ref,
    source_ref,
    kept_ref,
    cells_ref,
    added_ref,
    all_ref,
    m_ref,
    sem,
):
    links, _, species = mine_ref.shape[:3]
    blocks = species // N
    copy = pltpu.make_async_copy(source_hbm, source_ref, sem)
    copy.start()
    place = lax.axis_index("params")
    for k in range(links):
        for core, ref in enumerate((mine_ref, other_ref)):
            rows = pl.ds(place ^ (2 * k + core), species, stride=ROWS)
            if k == 0 and core == 0:
                cells_ref[rows, :] = conc_ref[...]
                added_ref[rows, :] = emis_ref[...]
            else:
                cells_ref[rows, :] = LEAST * jnp.exp(SPAN * decoded(ref[k, 0]))
                added_ref[rows, :] = decoded(ref[k, 1])

    def one(block, carry):
        tiles = [
            pl.ds(pl.multiple_of(order_ref[block * N + j] * ROWS, ROWS), ROWS) for j in range(N)
        ]
        for j in range(N):
            kept_ref[block * N + j] = order_ref[block * N + j]
        conc = [cells_ref[tile, :] for tile in tiles]
        minus_system(m_ref, conc, lambda i, j: rate_ref[block, i, j])
        inverted(m_ref)
        values = [-(cells_ref[tile, :] + added_ref[tile, :]) for tile in tiles]
        for i in range(0, N, 2):
            sums = [None, None]
            for j in range(N):
                pair = jnp.concatenate([m_ref[i * N + j], m_ref[(i + 1) * N + j]], 0)
                wide = pair.astype(jnp.bfloat16).astype(jnp.float32)
                factor_ref[block, j, i // 2] = wide
                for h in range(2):
                    term = wide[h * ROWS : (h + 1) * ROWS] * values[j]
                    sums[h] = term if sums[h] is None else sums[h] + term
            for h in range(2):
                all_ref[tiles[i + h], :] = sums[h]
        return carry

    lax.fori_loop(0, blocks, one, 0)
    new_ref[...] = all_ref[pl.ds(place, species, stride=ROWS), :]
    part_ref[...] = lane_sums(jnp.sum(all_ref[...].reshape(species, ROWS, LANES), axis=1))
    copy.wait()


def apply_kernel(
    order_ref,
    weights_ref,
    s_ref,
    t_ref,
    source_ref,
    a_ref,
    b_ref,
    half_0_ref,
    half_1_ref,
    factor_ref,
    conc_part_ref,
    out_ref,
    part_ref,
    even_ref,
    odd_ref,
):
    species = s_ref.shape[1]
    blocks = species // N
    tile = lax.axis_index("cols")
    odd = tile % 2 == 1
    relayed = is_late(tile) & ((tile % RUN == 0) | (tile % RUN == RUN - 1))
    extra_a = jnp.where(
        relayed,
        half_0_ref[species].astype(jnp.float32),
        a_ref[species].astype(jnp.float32)[:ROWS],
    )
    extra = jnp.where(odd, extra_a, b_ref[species].astype(jnp.float32)[:ROWS])
    first = lax.broadcasted_iota(jnp.int32, (ROWS, LANES), 0) < HALF
    upper = jnp.where(first, 0.0, extra + shifted(extra, HALF, 0))
    up_x = weights_ref[0]
    minus = (upper - weights_ref[1],) + tuple(-weights_ref[at] for at in range(2, 5))

    def values(block, j, ref):
        k = order_ref[block * N + j]
        wide_a = a_ref[k].astype(jnp.float32)
        wide_b = b_ref[k].astype(jnp.float32)
        for g, half_ref in enumerate((half_0_ref, half_1_ref)):
            from_a = jnp.where(
                relayed, half_ref[k].astype(jnp.float32), wide_a[g * ROWS : (g + 1) * ROWS]
            )
            from_b = wide_b[g * ROWS : (g + 1) * ROWS]
            a = jnp.where(odd, from_b, from_a)
            b = jnp.where(odd, from_a, from_b)
            inflow = up_x * a
            halo_0 = jnp.where(first, inflow, shifted(b, HALF, 0))
            halo_1 = jnp.where(first, up_x * (shifted(a, HALF, 0) - inflow), b)
            s = (t_ref[g, k] - upper * s_ref[g, k]) + halo_0
            s = moved(s, minus) - halo_1
            ref[j * 2 + g] = s - source_ref[g, k].astype(jnp.float32)

    def products(block, i, ref):
        sums = [[None, None], [None, None]]
        for j in range(N):
            wide = factor_ref[block, j, i]
            for h in range(2):
                f = wide[h * ROWS : (h + 1) * ROWS]
                for g in range(2):
                    term = f * ref[j * 2 + g]
                    sums[g][h] = term if sums[g][h] is None else sums[g][h] + term
        for h in range(2):
            k = order_ref[block * N + 2 * i + h]
            for g in range(2):
                out_ref[g, k] = sums[g][h]

    for j in range(N):
        values(0, j, even_ref)

    def two(pair, carry):
        block = 2 * pair
        for now, later, ref, other in (
            (block, block + 1, even_ref, odd_ref),
            (block + 1, lax.rem(block + 2, blocks), odd_ref, even_ref),
        ):
            for i in range(N // 2):
                products(now, i, ref)
                values(later, 2 * i, other)
                values(later, 2 * i + 1, other)
        return carry

    lax.fori_loop(0, blocks // 2, two, 0)
    tiles = part_ref.shape[0]
    for g in range(2):
        row = lane_sums(jnp.sum(out_ref[g], axis=1))[:1]
        part_ref[:, g, :] = jnp.broadcast_to(row, (tiles, LANES))
    part_ref[:, 2, :] = jnp.broadcast_to(conc_part_ref[:1], (tiles, LANES))


def means_kernel(scale, parts_ref, sens_ref, conc_ref):
    totals = jnp.sum(parts_ref[...], axis=0) * scale
    sens_ref[...] = totals[:2]
    conc_ref[...] = totals[2:3]


def near(value):
    return pltpu.with_memory_space_constraint(value, pltpu.VMEM)


def far(value):
    return pltpu.with_memory_space_constraint(value, pltpu.HBM)


def crossed(value, bits):
    return lax.ppermute(
        value, "params", [(i, i ^ bits) for i in range(lax.axis_size("params"))]
    )


def is_late(tile):
    return (tile // RUN) % 2 == 1


def edges(first):
    pairs = [(i, i + 1) for i in range(first, lax.axis_size("cols") - 1, 2)]
    return pairs + [(b, a) for a, b in pairs]


def leaps():
    return [
        (a, a - 1 if a < b else a + 1, b)
        for a, b in edges(1)
        if a // RUN != b // RUN and not is_late(a)
    ]


def passed(value, pairs):
    return lax.ppermute(value, "cols", pairs)


def step(
    concentration,
    emissions,
    rate_table,
    species_order,
    sensitivity,
    source_terms,
    courant_x,
    upwind_x,
    courant_y,
    upwind_y,
):
    blocks = rate_table.shape[0]
    groups, species, planes, layers, across = sensitivity.shape
    cells = planes * layers * across
    tiles = lax.axis_size("cols")
    s = sensitivity.reshape(groups, species, ROWS, LANES)
    source = source_terms.reshape(groups, species, ROWS, LANES)
    winds = [w.reshape(ROWS, LANES) for w in (courant_x, upwind_x, courant_y, upwind_y)]

    links = lax.axis_size("params") // 2
    message = pltpu.VMEM((species + 1, 2 * ROWS, LANES), jnp.bfloat16)
    packet = pl.pallas_call(
        packet_kernel,
        out_shape=pltpu.VMEM((2, species, LANES), jnp.int16),
        in_specs=[VMEM, VMEM],
        out_specs=VMEM,
        compiler_params=SMALL,
        name="packet",
    )(far(concentration), far(emissions))
    mine = [packet]
    for k in range(1, links):
        mine.append(crossed(packet, 2 * k))
    a, b, half_0, half_1, s_near, t_near, weights = pl.pallas_call(
        message_kernel,
        out_shape=(
            message,
            message,
            pltpu.VMEM((species + 1, ROWS, LANES), jnp.bfloat16),
            pltpu.VMEM((species, ROWS, LANES), jnp.bfloat16),
            pltpu.VMEM(s.shape, jnp.float32),
            pltpu.VMEM(s.shape, jnp.float32),
            pltpu.VMEM((5, ROWS, LANES), jnp.float32),
        ),
        in_specs=[ANY] * 5,
        out_specs=(VMEM,) * 7,
        scratch_shapes=[
            pltpu.VMEM((2, ROWS, LANES), jnp.float32),
            pltpu.VMEM((2, ROWS, LANES), jnp.int32),
            pltpu.SemaphoreType.DMA((4,)),
            pltpu.SemaphoreType.DMA((CHUNKS,)),
        ],
        compiler_params=SMALL,
        name="messages",
    )(*map(far, winds), far(s))
    far_edges = leaps()
    direct = [(u, v) for u, _, v in far_edges]
    a = passed(a, [edge for edge in edges(1) if edge not in direct])
    half_1 = passed(half_1, [(u, w) for u, w, _ in far_edges])
    half_0 = passed(half_0, direct)
    half_1 = passed(half_1, [(w, v) for _, w, v in far_edges])
    b = passed(b, edges(0))
    mine = jnp.stack(mine)
    other = crossed(mine, 1)

    factors, new_concentration, conc_part, source_near, order_near = pl.pallas_call(
        factor_kernel,
        out_shape=(
            pltpu.VMEM((blocks, N, N // 2, 2 * ROWS, LANES), jnp.float32),
            pltpu.VMEM((species, LANES), jnp.float32),
            pltpu.VMEM((ROWS, LANES), jnp.float32),
            pltpu.VMEM(source.shape, source.dtype),
            pltpu.SMEM(species_order.shape, jnp.int32),
        ),
        in_specs=[SMEM, SMEM, VMEM, VMEM, VMEM, VMEM, ANY],
        out_specs=(VMEM,) * 4 + (SMEM,),
        scratch_shapes=[
            pltpu.VMEM((species * ROWS, LANES), jnp.float32),
            pltpu.VMEM((species * ROWS, LANES), jnp.float32),
            pltpu.VMEM((species * ROWS, LANES), jnp.float32),
            pltpu.VMEM((N * N, ROWS, LANES), jnp.float32),
            pltpu.SemaphoreType.DMA,
        ],
        compiler_params=SMALL,
        name="factors",
    )(
        far(species_order),
        far(rate_table),
        near(mine),
        near(other),
        far(concentration),
        far(emissions),
        far(source),
    )

    new_sens, parts = pl.pallas_call(
        apply_kernel,
        out_shape=(
            pltpu.VMEM(s.shape, jnp.float32),
            pltpu.VMEM((tiles, 3, LANES), jnp.float32),
        ),
        in_specs=[SMEM] + [VMEM] * 10,
        out_specs=(VMEM, VMEM),
        scratch_shapes=[pltpu.VMEM((2 * N, ROWS, LANES), jnp.float32)] * 2,
        compiler_params=SMALL,
        name="apply",
    )(
        pltpu.with_memory_space_constraint(order_near, pltpu.SMEM),
        near(weights),
        near(s_near),
        near(t_near),
        near(source_near),
        near(a),
        near(b),
        near(half_0),
        near(half_1),
        near(factors),
        near(conc_part),
    )

    everything = lax.all_to_all(parts, "cols", 0, 0, tiled=True)
    sens_mean, conc_mean = pl.pallas_call(
        functools.partial(means_kernel, 1.0 / (cells * tiles)),
        out_shape=(
            jax.ShapeDtypeStruct((groups, species), jnp.float32),
            jax.ShapeDtypeStruct((1, species), jnp.float32),
        ),
        in_specs=[VMEM],
        out_specs=(VMEM, VMEM),
        compiler_params=SMALL,
        name="means",
    )(near(everything))
    return (
        new_concentration,
        new_sens.reshape(sensitivity.shape),
        sens_mean,
        conc_mean.reshape(species),
    )


def solution(mesh):
    in_specs = (
        P(None, ("cols", "params")),
        P(None, ("cols", "params")),
        P(),
        P(),
        P("params", None, "cols"),
        P("params", None, "cols"),
        P("cols"),
        P("cols"),
        P("cols"),
        P("cols"),
    )
    out_specs = (P(None, ("cols", "params")), P("params", None, "cols"), P("params"), P())
    return jax.shard_map(step, mesh=mesh, in_specs=in_specs, out_specs=out_specs, check_vma=False)
```

```python
import functools
import math

import jax
import jax.numpy as jnp
from jax import lax
from jax.experimental import pallas as pl
from jax.experimental.pallas import tpu as pltpu
from jax.sharding import PartitionSpec as P


ROWS, LANES = 8, 128
HALF = ROWS // 2
N = 16
CHUNKS = 8
RUN = 4
LEAST, SPAN = 0.2, math.log(25.0)
TOP, CENTRE = 65535.0, 32768.0
HIGHEST = lax.Precision.HIGHEST
VMEM = pl.BlockSpec(memory_space=pltpu.VMEM)
SMEM = pl.BlockSpec(memory_space=pltpu.SMEM)
ANY = pl.BlockSpec(memory_space=pl.ANY)
SMALL = pltpu.CompilerParams(vmem_limit_bytes=16 << 20)


def shifted(value, by, axis):
    return pltpu.roll(value, by % value.shape[axis], axis)


def coefficients(cx, ux, cy, uy):
    row = lax.broadcasted_iota(jnp.int32, (ROWS, LANES), 0)
    lane = lax.broadcasted_iota(jnp.int32, (ROWS, LANES), 1)
    first = row < HALF
    up_x = jnp.where(ux == 1, cx, 0.0)
    down_x = jnp.where(ux == 1, 0.0, cx)
    up_y = jnp.where(uy == 1, cy, 0.0)
    down_y = jnp.where(uy == 1, 0.0, cy)
    before = jnp.where(lane == 0, 0.0, up_y)
    leave = jnp.where(lane == LANES - 1, 0.0, shifted(up_y, -1, 1))
    after = jnp.where(lane == LANES - 1, 0.0, shifted(down_y, -1, 1))
    other = jnp.where(first, shifted(down_x, HALF, 0), up_x)
    leave_x = jnp.where(first, shifted(up_x, HALF, 0), 0.0)
    own = 1.0 - down_y - leave - down_x - leave_x
    return first, up_x, down_x, (own, other, before, after)


def moved(s, weights):
    own, other, before, after = weights
    return (
        own * s
        + other * shifted(s, HALF, 0)
        + before * shifted(s, 1, 1)
        + after * shifted(s, -1, 1)
    )


def inverted(m_ref):
    for k in range(0, N, 2):
        x = [m_ref[k * N + j] for j in range(N)]
        y = [m_ref[(k + 1) * N + j] for j in range(N)]
        p = 1.0 / x[k]
        x = [p if j == k else x[j] * p for j in range(N)]
        e = y[k]
        y = [e * -x[j] if j == k else y[j] - e * x[j] for j in range(N)]
        p = 1.0 / y[k + 1]
        y = [p if j == k + 1 else y[j] * p for j in range(N)]
        e = x[k + 1]
        x = [e * -y[j] if j == k + 1 else x[j] - e * y[j] for j in range(N)]
        minus_x = {j: -x[j] for j in (k, k + 1)}
        minus_y = {j: -y[j] for j in (k, k + 1)}
        for i in range(N):
            if i in (k, k + 1):
                continue
            a = m_ref[i * N + k]
            b = m_ref[i * N + k + 1]
            for j in range(N):
                if j in (k, k + 1):
                    m_ref[i * N + j] = a * minus_x[j] + b * minus_y[j]
                else:
                    m_ref[i * N + j] = m_ref[i * N + j] - (a * x[j] + b * y[j])
        for j in range(N):
            m_ref[k * N + j] = x[j]
            m_ref[(k + 1) * N + j] = y[j]


def minus_system(m_ref, conc, rate):
    for i in range(N):
        row = [rate(i, j) * conc[j] for j in range(N)]
        total = row[0]
        for j in range(1, N):
            total = total + row[j]
        for j in range(N):
            m_ref[i * N + j] = row[j] - (1.0 + total) if i == j else row[j]


def lane_sums(rows):
    ones = jnp.ones((ROWS, LANES), jnp.float32)
    return lax.dot_general(ones, rows, (((1,), (1,)), ((), ())), precision=HIGHEST)


def coded(unit):
    steps = jnp.clip(jnp.floor(unit * TOP + 0.5), 0.0, TOP) - CENTRE
    return steps.astype(jnp.int32).astype(jnp.int16)


def decoded(code):
    return (code.astype(jnp.int32).astype(jnp.float32) + CENTRE) * (1.0 / TOP)


def packet_kernel(conc_ref, emis_ref, packet_ref, near_ref):
    near_ref[0] = conc_ref[...]
    near_ref[1] = emis_ref[...]
    packet_ref[0] = coded(jnp.log(conc_ref[...] * (1.0 / LEAST)) * (1.0 / SPAN))
    packet_ref[1] = coded(emis_ref[...])


def message_kernel(
    cx_hbm,
    ux_hbm,
    cy_hbm,
    uy_hbm,
    s_hbm,
    order_hbm,
    rate_hbm,
    a_ref,
    b_ref,
    half_0_ref,
    half_1_ref,
    s_ref,
    t_ref,
    weights_ref,
    order_ref,
    rate_ref,
    reals_ref,
    flags_ref,
    wind_sem,
    sems,
    table_sem,
):
    species = s_ref.shape[1]
    size = species // CHUNKS

    def copy(c):
        part = (slice(None), pl.ds(c * size, size))
        return pltpu.make_async_copy(s_hbm.at[part], s_ref.at[part], sems.at[c])

    winds = [
        pltpu.make_async_copy(source, target, wind_sem.at[at])
        for at, (source, target) in enumerate(
            (
                (cx_hbm, reals_ref.at[0]),
                (ux_hbm, flags_ref.at[0]),
                (cy_hbm, reals_ref.at[1]),
                (uy_hbm, flags_ref.at[1]),
            )
        )
    ]
    tables = (
        pltpu.make_async_copy(order_hbm, order_ref, table_sem.at[0]),
        pltpu.make_async_copy(rate_hbm, rate_ref, table_sem.at[1]),
    )
    for wind in winds:
        wind.start()
    for c in range(CHUNKS):
        copy(c).start()
    for table in tables:
        table.start()
    for wind in winds:
        wind.wait()
    first, up_x, down_x, weights = coefficients(
        reals_ref[0], flags_ref[0], reals_ref[1], flags_ref[1]
    )
    down = jnp.where(first, down_x, 0.0)
    for at, weight in enumerate((up_x, *weights)):
        weights_ref[at] = weight
    high = up_x.astype(jnp.bfloat16).astype(jnp.float32)
    low = up_x - high
    both = jnp.where(first, high, shifted(low, HALF, 0))
    extra = jnp.concatenate([both, jnp.zeros_like(both)], 0).astype(jnp.bfloat16)
    odd = lax.axis_index("cols") % 2 == 1
    a_ref[species] = extra
    b_ref[species] = extra
    half_0_ref[species] = extra[:ROWS]

    def work(right_ref, left_ref, to_right):
        def chunk(c, carry):
            copy(c).wait()
            for at in range(size):
                k = c * size + at
                rights, lefts = [], []
                for g in range(2):
                    s = s_ref[g, k]
                    t = moved(s, weights)
                    t_ref[g, k] = t
                    rights.append(jnp.where(first, shifted(s, HALF, 0), t))
                    lefts.append(jnp.where(first, down * s, shifted(down * t, HALF, 0)))
                right_ref[k] = jnp.concatenate(rights, 0).astype(jnp.bfloat16)
                left_ref[k] = jnp.concatenate(lefts, 0).astype(jnp.bfloat16)
                halves = rights if to_right else lefts
                half_0_ref[k] = halves[0].astype(jnp.bfloat16)
                half_1_ref[k] = halves[1].astype(jnp.bfloat16)
            return carry

        lax.fori_loop(0, CHUNKS, chunk, 0)

    @pl.when(odd)
    def _():
        work(a_ref, b_ref, True)

    @pl.when(jnp.logical_not(odd))
    def _():
        work(b_ref, a_ref, False)

    for table in tables:
        table.wait()


def factor_kernel(
    order_ref,
    rate_ref,
    mine_ref,
    other_ref,
    own_ref,
    source_hbm,
    factor_ref,
    new_ref,
    part_ref,
    source_ref,
    cells_ref,
    added_ref,
    all_ref,
    m_ref,
    sem,
):
    links, _, species = mine_ref.shape[:3]
    blocks = species // N
    copy = pltpu.make_async_copy(source_hbm, source_ref, sem)
    copy.start()
    place = lax.axis_index("params")
    for k in range(links):
        for core, ref in enumerate((mine_ref, other_ref)):
            rows = pl.ds(place ^ (2 * k + core), species, stride=ROWS)
            if k == 0 and core == 0:
                cells_ref[rows, :] = own_ref[0]
                added_ref[rows, :] = own_ref[1]
            else:
                cells_ref[rows, :] = LEAST * jnp.exp(SPAN * decoded(ref[k, 0]))
                added_ref[rows, :] = decoded(ref[k, 1])

    def one(block, carry):
        tiles = [
            pl.ds(pl.multiple_of(order_ref[block * N + j] * ROWS, ROWS), ROWS) for j in range(N)
        ]
        conc = [cells_ref[tile, :] for tile in tiles]
        minus_system(m_ref, conc, lambda i, j: rate_ref[block, i, j])
        inverted(m_ref)
        values = [-(cells_ref[tile, :] + added_ref[tile, :]) for tile in tiles]
        for i in range(0, N, 2):
            sums = [None, None]
            for j in range(N):
                pair = jnp.concatenate([m_ref[i * N + j], m_ref[(i + 1) * N + j]], 0)
                wide = pair.astype(jnp.bfloat16).astype(jnp.float32)
                factor_ref[block, j, i // 2] = wide
                for h in range(2):
                    term = wide[h * ROWS : (h + 1) * ROWS] * values[j]
                    sums[h] = term if sums[h] is None else sums[h] + term
            for h in range(2):
                all_ref[tiles[i + h], :] = sums[h]
        return carry

    lax.fori_loop(0, blocks, one, 0)
    new_ref[...] = all_ref[pl.ds(place, species, stride=ROWS), :]
    part_ref[...] = lane_sums(jnp.sum(all_ref[...].reshape(species, ROWS, LANES), axis=1))
    copy.wait()


def apply_kernel(
    order_ref,
    weights_ref,
    s_ref,
    t_ref,
    source_ref,
    a_ref,
    b_ref,
    half_0_ref,
    half_1_ref,
    factor_ref,
    conc_part_ref,
    out_ref,
    part_ref,
    even_ref,
    odd_ref,
):
    species = s_ref.shape[1]
    blocks = species // N
    tile = lax.axis_index("cols")
    odd = tile % 2 == 1
    relayed = is_late(tile) & ((tile % RUN == 0) | (tile % RUN == RUN - 1))
    extra_a = jnp.where(
        relayed,
        half_0_ref[species].astype(jnp.float32),
        a_ref[species].astype(jnp.float32)[:ROWS],
    )
    extra = jnp.where(odd, extra_a, b_ref[species].astype(jnp.float32)[:ROWS])
    first = lax.broadcasted_iota(jnp.int32, (ROWS, LANES), 0) < HALF
    upper = jnp.where(first, 0.0, extra + shifted(extra, HALF, 0))
    up_x = weights_ref[0]
    minus = (upper - weights_ref[1],) + tuple(-weights_ref[at] for at in range(2, 5))

    def values(block, j, ref):
        k = order_ref[block * N + j]
        wide_a = a_ref[k].astype(jnp.float32)
        wide_b = b_ref[k].astype(jnp.float32)
        for g, half_ref in enumerate((half_0_ref, half_1_ref)):
            from_a = jnp.where(
                relayed, half_ref[k].astype(jnp.float32), wide_a[g * ROWS : (g + 1) * ROWS]
            )
            from_b = wide_b[g * ROWS : (g + 1) * ROWS]
            a = jnp.where(odd, from_b, from_a)
            b = jnp.where(odd, from_a, from_b)
            inflow = up_x * a
            halo_0 = jnp.where(first, inflow, shifted(b, HALF, 0))
            halo_1 = jnp.where(first, up_x * (shifted(a, HALF, 0) - inflow), b)
            s = (t_ref[g, k] - upper * s_ref[g, k]) + halo_0
            s = moved(s, minus) - halo_1
            ref[j * 2 + g] = s - source_ref[g, k].astype(jnp.float32)

    def products(block, i, ref):
        sums = [[None, None], [None, None]]
        for j in range(N):
            wide = factor_ref[block, j, i]
            for h in range(2):
                f = wide[h * ROWS : (h + 1) * ROWS]
                for g in range(2):
                    term = f * ref[j * 2 + g]
                    sums[g][h] = term if sums[g][h] is None else sums[g][h] + term
        for h in range(2):
            k = order_ref[block * N + 2 * i + h]
            for g in range(2):
                out_ref[g, k] = sums[g][h]

    for j in range(N):
        values(0, j, even_ref)

    def two(pair, carry):
        block = 2 * pair
        for now, later, ref, other in (
            (block, block + 1, even_ref, odd_ref),
            (block + 1, lax.rem(block + 2, blocks), odd_ref, even_ref),
        ):
            for i in range(N // 2):
                products(now, i, ref)
                values(later, 2 * i, other)
                values(later, 2 * i + 1, other)
        return carry

    lax.fori_loop(0, blocks // 2, two, 0)
    tiles = part_ref.shape[0]
    for g in range(2):
        row = lane_sums(jnp.sum(out_ref[g], axis=1))[:1]
        part_ref[:, g, :] = jnp.broadcast_to(row, (tiles, LANES))
    part_ref[:, 2, :] = jnp.broadcast_to(conc_part_ref[:1], (tiles, LANES))


def means_kernel(scale, parts_ref, sens_ref, conc_ref):
    totals = jnp.sum(parts_ref[...], axis=0) * scale
    sens_ref[...] = totals[:2]
    conc_ref[...] = totals[2:3]


def near(value):
    return pltpu.with_memory_space_constraint(value, pltpu.VMEM)


def scalars(value):
    return pltpu.with_memory_space_constraint(value, pltpu.SMEM)


def far(value):
    return pltpu.with_memory_space_constraint(value, pltpu.HBM)


def crossed(value, bits):
    return lax.ppermute(
        value, "params", [(i, i ^ bits) for i in range(lax.axis_size("params"))]
    )


def is_late(tile):
    return (tile // RUN) % 2 == 1


def edges(first):
    pairs = [(i, i + 1) for i in range(first, lax.axis_size("cols") - 1, 2)]
    return pairs + [(b, a) for a, b in pairs]


def leaps():
    return [
        (a, a - 1 if a < b else a + 1, b)
        for a, b in edges(1)
        if a // RUN != b // RUN and not is_late(a)
    ]


def passed(value, pairs):
    return lax.ppermute(value, "cols", pairs)


def step(
    concentration,
    emissions,
    rate_table,
    species_order,
    sensitivity,
    source_terms,
    courant_x,
    upwind_x,
    courant_y,
    upwind_y,
):
    blocks = rate_table.shape[0]
    groups, species, planes, layers, across = sensitivity.shape
    cells = planes * layers * across
    tiles = lax.axis_size("cols")
    s = sensitivity.reshape(groups, species, ROWS, LANES)
    source = source_terms.reshape(groups, species, ROWS, LANES)
    winds = [w.reshape(ROWS, LANES) for w in (courant_x, upwind_x, courant_y, upwind_y)]

    links = lax.axis_size("params") // 2
    message = pltpu.VMEM((species + 1, 2 * ROWS, LANES), jnp.bfloat16)
    packet, cells_near = pl.pallas_call(
        packet_kernel,
        out_shape=(
            pltpu.VMEM((2, species, LANES), jnp.int16),
            pltpu.VMEM((2, species, LANES), jnp.float32),
        ),
        in_specs=[VMEM, VMEM],
        out_specs=(VMEM, VMEM),
        compiler_params=SMALL,
        name="packet",
    )(far(concentration), far(emissions))
    mine = [packet]
    for k in range(1, links):
        mine.append(crossed(packet, 2 * k))
    a, b, half_0, half_1, s_near, t_near, weights, order_near, rate_near = pl.pallas_call(
        message_kernel,
        out_shape=(
            message,
            message,
            pltpu.VMEM((species + 1, ROWS, LANES), jnp.bfloat16),
            pltpu.VMEM((species, ROWS, LANES), jnp.bfloat16),
            pltpu.VMEM(s.shape, jnp.float32),
            pltpu.VMEM(s.shape, jnp.float32),
            pltpu.VMEM((5, ROWS, LANES), jnp.float32),
            pltpu.SMEM(species_order.shape, jnp.int32),
            pltpu.SMEM(rate_table.shape, jnp.float32),
        ),
        in_specs=[ANY] * 7,
        out_specs=(VMEM,) * 7 + (SMEM,) * 2,
        scratch_shapes=[
            pltpu.VMEM((2, ROWS, LANES), jnp.float32),
            pltpu.VMEM((2, ROWS, LANES), jnp.int32),
            pltpu.SemaphoreType.DMA((4,)),
            pltpu.SemaphoreType.DMA((CHUNKS,)),
            pltpu.SemaphoreType.DMA((2,)),
        ],
        compiler_params=SMALL,
        name="messages",
    )(*map(far, winds), far(s), far(species_order), far(rate_table))
    far_edges = leaps()
    direct = [(u, v) for u, _, v in far_edges]
    a = passed(a, [edge for edge in edges(1) if edge not in direct])
    half_1 = passed(half_1, [(u, w) for u, w, _ in far_edges])
    half_0 = passed(half_0, direct)
    half_1 = passed(half_1, [(w, v) for _, w, v in far_edges])
    b = passed(b, edges(0))
    mine = jnp.stack(mine)
    other = crossed(mine, 1)

    factors, new_concentration, conc_part, source_near = pl.pallas_call(
        factor_kernel,
        out_shape=(
            pltpu.VMEM((blocks, N, N // 2, 2 * ROWS, LANES), jnp.float32),
            pltpu.VMEM((species, LANES), jnp.float32),
            pltpu.VMEM((ROWS, LANES), jnp.float32),
            pltpu.VMEM(source.shape, source.dtype),
        ),
        in_specs=[SMEM, SMEM, VMEM, VMEM, VMEM, ANY],
        out_specs=(VMEM,) * 4,
        scratch_shapes=[
            pltpu.VMEM((species * ROWS, LANES), jnp.float32),
            pltpu.VMEM((species * ROWS, LANES), jnp.float32),
            pltpu.VMEM((species * ROWS, LANES), jnp.float32),
            pltpu.VMEM((N * N, ROWS, LANES), jnp.float32),
            pltpu.SemaphoreType.DMA,
        ],
        compiler_params=SMALL,
        name="factors",
    )(
        scalars(order_near),
        scalars(rate_near),
        near(mine),
        near(other),
        near(cells_near),
        far(source),
    )

    new_sens, parts = pl.pallas_call(
        apply_kernel,
        out_shape=(
            pltpu.VMEM(s.shape, jnp.float32),
            pltpu.VMEM((tiles, 3, LANES), jnp.float32),
        ),
        in_specs=[SMEM] + [VMEM] * 10,
        out_specs=(VMEM, VMEM),
        scratch_shapes=[pltpu.VMEM((2 * N, ROWS, LANES), jnp.float32)] * 2,
        compiler_params=SMALL,
        name="apply",
    )(
        scalars(order_near),
        near(weights),
        near(s_near),
        near(t_near),
        near(source_near),
        near(a),
        near(b),
        near(half_0),
        near(half_1),
        near(factors),
        near(conc_part),
    )

    everything = lax.all_to_all(parts, "cols", 0, 0, tiled=True)
    sens_mean, conc_mean = pl.pallas_call(
        functools.partial(means_kernel, 1.0 / (cells * tiles)),
        out_shape=(
            jax.ShapeDtypeStruct((groups, species), jnp.float32),
            jax.ShapeDtypeStruct((1, species), jnp.float32),
        ),
        in_specs=[VMEM],
        out_specs=(VMEM, VMEM),
        compiler_params=SMALL,
        name="means",
    )(near(everything))
    return (
        new_concentration,
        new_sens.reshape(sensitivity.shape),
        sens_mean,
        conc_mean.reshape(species),
    )


def solution(mesh):
    in_specs = (
        P(None, ("cols", "params")),
        P(None, ("cols", "params")),
        P(),
        P(),
        P("params", None, "cols"),
        P("params", None, "cols"),
        P("cols"),
        P("cols"),
        P("cols"),
        P("cols"),
    )
    out_specs = (P(None, ("cols", "params")), P("params", None, "cols"), P("params"), P())
    return jax.shard_map(step, mesh=mesh, in_specs=in_specs, out_specs=out_specs, check_vma=False)
```
